32 devices in a mesh: tile: 8 (over y, x, core), lev: 4 (over z).
Axes of the slice: x: 2, y: 2, z: 4, core: 2. Of those that a mesh axis runs over, the one named last changes fastest.
Arguments:
- members_pert: bfloat16 [64, 16, 32768], P('lev', None, 'tile'), may hold values from -4 to 4
- coarse_pert: bfloat16 [64, 8, 2048], P('lev', None, 'tile'), may hold values from -6 to 6
- member_ctrl: bfloat16 [64, 16, 2048], P('lev', None, 'tile'), may hold values from -6 to 6
- coarse_ctrl: bfloat16 [64, 8, 2048], P('lev', None, 'tile'), may hold values from -6 to 6
- vert_loc: float32 [64, 64], replicated, may hold values from -1.5 to 1.5, as said below
- stencil: int32 [4, 32768], P(None, 'tile'), may hold values from 0 to 383, as said below
- interp_w: bfloat16 [4, 32768], P(None, 'tile'), may hold values from 0 to 1, as said below
Outputs:
- member_out: float32 [64, 16, 2048], P('lev', None, 'tile')
- coarse_out: float32 [64, 8, 2048], P('lev', None, 'tile')
The draws below stay inside these ranges and needn't reach their ends.
Inputs may be any that keep to these rules, and one draw needn't show every extreme that they name: vert_loc[i, j] is zero where |i - j| > 4, and nonzero where |i - j| = 4. stencil indexes a window of 384 coarse cells of the fine cell's tile index: the last 64 coarse cells of the tile index before it (the first one's predecessor is the last), its own 256 cells, then the first 64 cells of the tile index after it; the four corners of a fine cell are distinct. `interp_w`: the four weights of a fine cell are nonnegative and sum to one up to rounding.
All inputs are finite; a program needn't handle non-finite values.
Results may differ from the reference program's by a relative error of at most 0.013.
Values may be sent and summed in bfloat16 or wider, within the bound.
A program may use at most 64 MiB of HBM per device.

```python
import jax
import jax.numpy as jnp
from jax import lax

MEMBERS = 16
COARSE_MEMBERS = 8
HB = 4
CW = 64
CR = 4
LEV = 64
NCD = 256
NFD = 4096
NC = 2048
NF = 32768
N_TILE = 8


def draw_vert_loc(key, part):
    first_key, second_key = jax.random.split(key)
    rows = jnp.arange(LEV, dtype=jnp.int32)[:, None]
    columns = jnp.arange(LEV, dtype=jnp.int32)[None, :]
    distance = jnp.abs(rows - columns)
    offdiag = jnp.clip(0.35 * jax.random.normal(first_key, (LEV, LEV), jnp.float32), -1.5, 1.5)
    offdiag = jnp.where(jnp.abs(offdiag) < 0.05, 0.05, offdiag)
    diagonal = 1.0 + jax.random.uniform(second_key, (LEV, LEV), jnp.float32, 0.0, 0.5)
    return jnp.where(distance == 0, diagonal, jnp.where(distance <= HB, offdiag, 0.0)).astype(jnp.float32)


def draw_stencil(key, part):
    row_key, col_key = jax.random.split(key)
    local = jnp.arange(NF, dtype=jnp.int32) % NFD
    fine_row = local // (4 * CW)
    fine_col = local % (4 * CW)
    row_base = jnp.clip((fine_row - 2) // 4 + jax.random.randint(row_key, (NF,), -1, 2), -1, CR - 1)
    col_base = jnp.clip((fine_col - 2) // 4 + jax.random.randint(col_key, (NF,), -1, 2), 0, CW - 2)
    corner = (row_base + 1) * CW + col_base
    return jnp.stack([corner, corner + 1, corner + CW, corner + CW + 1]).astype(jnp.int32)


def draw_interp_w(key, part):
    along_key, across_key = jax.random.split(key)
    along = jax.random.uniform(along_key, (NF,), jnp.float32)
    across = jax.random.uniform(across_key, (NF,), jnp.float32)
    weights = jnp.stack([(1.0 - along) * (1.0 - across), along * (1.0 - across), (1.0 - along) * across, along * across])
    return weights.astype(jnp.bfloat16)


def shard_levels(key, dims, pieces, low, top_value):
    gain = 1.0
    for dim, parts in pieces:
        heights = jax.random.uniform(jax.random.fold_in(jax.random.fold_in(key, 6), dim), (parts,), jnp.float32, low / len(pieces), top_value / len(pieces))
        gain = gain * jnp.repeat(jnp.exp(heights), dims[dim] // parts).reshape((-1,) + (1,) * (len(dims) - 1 - dim))
    return gain


def noise(own_key, shape, spread, reach, shards=(), kind=jnp.bfloat16):
    array = spread * jax.random.normal(own_key, shape, jnp.float32)
    if shards:
        array = array * shard_levels(own_key, shape, shards, -0.22, 0.18)
    return jnp.clip(array, -reach, reach).astype(kind)


def setup_inputs(seed: int = 0) -> dict:
    splits = jax.random.split(jax.random.key(seed), 8)
    members_pert = noise(splits[0], (LEV, MEMBERS, NF), 0.3, 4.0, ((0, 4), (2, 8)))
    coarse_pert = noise(splits[1], (LEV, COARSE_MEMBERS, NC), 0.4, 6.0, ((0, 4), (2, 8)))
    member_ctrl = noise(splits[2], (LEV, MEMBERS, NC), 1.0, 6.0, ((0, 4), (2, 8)))
    coarse_ctrl = noise(splits[3], (LEV, COARSE_MEMBERS, NC), 1.0, 6.0, ((0, 4), (2, 8)))
    vert_loc = draw_vert_loc(jax.random.fold_in(splits[7], 71), 0)
    stencil = draw_stencil(jax.random.fold_in(splits[7], 71), 0)
    interp_w = draw_interp_w(jax.random.fold_in(splits[7], 71), 0)
    return {"members_pert": members_pert, "coarse_pert": coarse_pert, "member_ctrl": member_ctrl, "coarse_ctrl": coarse_ctrl, "vert_loc": vert_loc, "stencil": stencil, "interp_w": interp_w}


def reference(members_pert, coarse_pert, member_ctrl, coarse_ctrl, vert_loc, stencil, interp_w):
    highest = lax.Precision.HIGHEST
    loc_members = jnp.einsum("ij,jkc->ikc", vert_loc, member_ctrl.astype(jnp.float32), precision=highest).astype(jnp.bfloat16)
    loc_coarse = jnp.einsum("ij,jkc->ikc", vert_loc, coarse_ctrl.astype(jnp.float32), precision=highest).astype(jnp.bfloat16)
    combined = jnp.sum(coarse_pert.astype(jnp.float32) * loc_coarse.astype(jnp.float32), axis=1).astype(jnp.bfloat16)
    fields = jnp.concatenate([loc_members, combined[:, None, :]], axis=1)
    levels = fields.shape[0]
    kinds = fields.shape[1]
    blocks = fields.reshape(levels, kinds, N_TILE, NCD)
    window = jnp.concatenate([jnp.roll(blocks, 1, axis=2)[..., NCD - CW:], blocks, jnp.roll(blocks, -1, axis=2)[..., :CW]], axis=3)
    window = jnp.moveaxis(window, 2, 0)
    window_span = window.shape[3]

    def one_tile(tile_index):
        local_window = lax.dynamic_index_in_dim(window, tile_index, 0, keepdims=False)
        first = (tile_index * NFD).astype(jnp.int32)
        corners = lax.dynamic_slice_in_dim(stencil, first, NFD, 1)
        weights = lax.dynamic_slice_in_dim(interp_w, first, NFD, 1).astype(jnp.float32)
        pert = lax.dynamic_slice_in_dim(members_pert, first, NFD, 2).astype(jnp.float32)
        interp = jnp.zeros((levels, kinds, NFD), jnp.float32)
        for corner in range(4):
            interp = interp + weights[corner][None, None, :] * local_window[:, :, corners[corner]].astype(jnp.float32)
        increment = jnp.sum(pert * interp[:, :MEMBERS], axis=1) + interp[:, MEMBERS]
        adjoint = jnp.concatenate([pert * increment[:, None, :], increment[:, None, :]], axis=1)
        adjoint = adjoint.astype(jnp.bfloat16).astype(jnp.float32)
        coarse_adjoint = jnp.zeros((levels, kinds, window_span), jnp.float32)
        for corner in range(4):
            coarse_adjoint = coarse_adjoint.at[:, :, corners[corner]].add(weights[corner][None, None, :] * adjoint)
        return coarse_adjoint

    backs = lax.map(one_tile, jnp.arange(N_TILE, dtype=jnp.int32))
    own_cells = backs[..., CW:CW + NCD]
    left_rim = backs[..., :CW]
    right_rim = backs[..., CW + NCD:]
    own_cells = own_cells.at[..., NCD - CW:].add(jnp.roll(left_rim, -1, axis=0))
    own_cells = own_cells.at[..., :CW].add(jnp.roll(right_rim, 1, axis=0))
    gathered = jnp.moveaxis(own_cells, 0, 2).reshape(levels, kinds, N_TILE * NCD)
    adjoint_ctrl = jnp.concatenate([gathered[:, :MEMBERS], coarse_pert.astype(jnp.float32) * gathered[:, MEMBERS:MEMBERS + 1]], axis=1)
    result = jnp.einsum("ij,ikc->jkc", vert_loc, adjoint_ctrl, precision=highest)
    return result[:, :MEMBERS], result[:, MEMBERS:]
```

```python
import functools

import jax
import jax.numpy as jnp
from jax import lax
from jax.experimental import pallas as pl
from jax.experimental.pallas import tpu as pltpu
from jax.sharding import PartitionSpec as P

HB = 4
CW = 64
LANE = 128
WIDE = 8
DEEP = 8
MESH = pl.DeviceIdType.MESH
F32 = jnp.float32
BF16 = jnp.bfloat16

DIRECTIONS = ((0, -1), (0, 1), (-1, 0), (1, 0), (-1, -1), (1, -1), (-1, 1), (1, 1))


def pairs_of(rows):
    half = HB // 2
    return [(b + k, b + k + half) for b in range(0, rows, HB) for k in range(half)]


def dims(rows, members, group, cells):
    comb_at = (rows - HB) * members
    packed = comb_at // 2 + rows + HB * members // 2
    return comb_at, packed


def fold(values):
    row = lax.broadcasted_iota(jnp.int32, (8, LANE), 0)
    for stride in (1, 2, 4):
        even = (row // stride) % 2 == 0
        values = [
            jnp.where(even, a, b) + pltpu.roll(jnp.where(even, b, a), stride, 0)
            for a, b in zip(values[0::2], values[1::2])
        ]
    return values[0]


def kernel(
    tiles, levs, pert_hbm, cp_hbm, mc_hbm, cc_hbm, vert_hbm, st_hbm, w_hbm, xm, xc, bm, bc,
    mc, cc, cp, pert, vert, st, w, matrix, am, ac, rim_m, rim_c, rim_p, pk, rt, rd,
    fld, fld_rim, adj, line, acc_rim, out_own, out_rim, acc_own, r_tile, r_lev, r_diag,
    load_sem, send, recv1, recv2,
):
    rows, members, cells = mc_hbm.shape
    group = cc_hbm.shape[1]
    total_levels = vert_hbm.shape[0]
    fine = pert_hbm.shape[2]
    span = cells + LANE
    window = rows + 2 * HB
    edge = HB * members + rows
    last = cells - LANE
    comb_at, packed = dims(rows, members, group, cells)
    pcomb_at = comb_at // 2
    low_at = comb_at + rows
    tail_at = comb_at - HB * members
    ptail_at = pcomb_at - HB * members // 2
    pedge = HB * members // 2 + rows
    pairs = pairs_of(rows)
    half = HB // 2
    kinds = members + 2 * group

    def level_at(i):
        return (i - HB) * members if i >= HB else low_at + i * members

    t = lax.axis_index("tile")
    v = lax.axis_index("lev")
    first = v * rows
    has = {-1: v > 0, 0: None, 1: v < levs - 1}
    beside = {-1: jnp.where(t == 0, tiles - 1, t - 1), 0: t, 1: jnp.where(t == tiles - 1, 0, t + 1)}

    def when(dl, action):
        if dl == 0:
            action()
        else:
            pl.when(has[dl])(action)

    def begin(copies):
        for dl, copy in copies:
            when(dl, copy.start)

    def settle(ref, sem):
        pltpu.make_async_copy(ref, ref, sem).wait()

    def filler(count):
        return pert.at[0, :, pl.ds(0, count // members)]

    def drain(ref, count):
        settle(ref, send.at[0])
        when(1, lambda: settle(filler(count), send.at[1]))
        when(-1, lambda: settle(filler(count), send.at[2]))

    own = pl.ds(HB, rows)
    loads = [
        pltpu.make_async_copy(mc_hbm, mc.at[own], load_sem.at[0]),
        pltpu.make_async_copy(cc_hbm, cc.at[own], load_sem.at[1]),
        pltpu.make_async_copy(cp_hbm, cp.at[own], load_sem.at[2]),
        pltpu.make_async_copy(st_hbm, st, load_sem.at[3]),
        pltpu.make_async_copy(w_hbm, w, load_sem.at[4]),
        pltpu.make_async_copy(vert_hbm, vert, load_sem.at[5]),
        pltpu.make_async_copy(pert_hbm, pert, load_sem.at[6]),
    ]
    for load in loads[:3]:
        load.start()

    barrier = pltpu.get_barrier_semaphore()
    for dt, dl in DIRECTIONS:
        when(
            dl,
            lambda dt=dt, dl=dl: pl.semaphore_signal(
                barrier, inc=1, device_id=(beside[dt], v + dl), device_id_type=MESH
            ),
        )
    for load in loads[3:]:
        load.start()

    def remote(src, dst, send_at, recv_at, dt, dl):
        return dl, pltpu.make_async_remote_copy(
            src_ref=src, dst_ref=dst, send_sem=send_at, recv_sem=recv_at,
            device_id=(beside[dt], v + dl), device_id_type=MESH,
        )

    level_src = {1: rows, -1: HB}
    level_dst = {1: 0, -1: HB + rows}
    entry_src = {1: len(pairs) - half, -1: 0}
    tile_row = {1: ptail_at, -1: pcomb_at}
    lev_row = {1: tail_at, -1: comb_at}
    lev1, late, tile1, diag1, tile2, diag2, lev2 = [], [], [], [], [], [], []
    for dl in (-1, 1):
        floor = (1 - dl) // 2
        for buf, copies, at in ((mc, lev1, 0), (cc, lev1, 0), (cp, late, 5)):
            copies.append(remote(
                buf.at[pl.ds(level_src[dl], HB)], buf.at[pl.ds(level_dst[dl], HB)],
                send.at[1 + floor], recv1.at[at + floor], 0, dl))
        lev2.append(remote(
            out_own.at[pl.ds(lev_row[dl], edge)], r_lev.at[floor],
            send.at[1 + floor], recv2.at[floor], 0, dl))
        for dt in (-1, 1):
            side = (1 + dt) // 2
            diag1.append(remote(
                pk.at[side, pl.ds(entry_src[dl], half)], rd.at[floor, side],
                send.at[1 + floor], recv1.at[2 + floor], dt, dl))
            diag2.append(remote(
                out_rim.at[side, pl.ds(tile_row[dl], pedge)], r_diag.at[floor, side],
                send.at[1 + floor], recv2.at[2 + floor], dt, dl))
    for dt in (-1, 1):
        side = (1 + dt) // 2
        tile1.append(remote(pk.at[side], rt.at[side], send.at[0], recv1.at[4], dt, 0))
        tile2.append(remote(out_rim.at[side], r_tile.at[side], send.at[0], recv2.at[4], dt, 0))
    near = HB * (members + group) * cells
    extra = HB * group * cells

    @pl.when(v == 0)
    def _():
        for buf in (mc, cc, cp):
            buf[0:HB] = jnp.zeros((HB,) + buf.shape[1:], BF16)
        rd[0] = jnp.zeros(rd.shape[1:], BF16)
        r_lev[0] = jnp.zeros(r_lev.shape[1:], BF16)
        r_diag[0] = jnp.zeros(r_diag.shape[1:], BF16)

    @pl.when(v == levs - 1)
    def _():
        for buf in (mc, cc, cp):
            buf[HB + rows :] = jnp.zeros((HB,) + buf.shape[1:], BF16)
        rd[1] = jnp.zeros(rd.shape[1:], BF16)
        r_lev[1] = jnp.zeros(r_lev.shape[1:], BF16)
        r_diag[1] = jnp.zeros(r_diag.shape[1:], BF16)

    def lower(shape):
        return lax.broadcasted_iota(jnp.int32, shape, len(shape) - 1) < CW

    def turned(value):
        return pltpu.roll(value, CW, 1)

    for load in loads[:3]:
        load.wait()
    neighbours = 2 + 3 * jnp.where(v > 0, 1, 0) + 3 * jnp.where(v < levs - 1, 1, 0)
    pl.semaphore_wait(barrier, neighbours)
    begin(lev1)
    for k, (a, b) in enumerate(pairs):
        for buf, r0, rn in ((mc, 0, members), (cc, members, group), (cp, members + group, group)):
            low = lower((rn, LANE))
            near_a, near_b = (buf[HB + i, :, 0:LANE].astype(F32) for i in (a, b))
            far_a, far_b = (buf[HB + i, :, last:].astype(F32) for i in (a, b))
            pk[0, k, r0 : r0 + rn, :] = jnp.where(low, near_a, turned(near_b)).astype(BF16)
            pk[1, k, r0 : r0 + rn, :] = jnp.where(low, turned(far_b), far_a).astype(BF16)
    begin(diag1 + tile1)
    for load in loads[3:6]:
        load.wait()
    pack = 16
    base_rows = lax.broadcasted_iota(jnp.int32, (pack, LANE), 0).astype(jnp.int16)

    def build(step, carry):
        lanes = pl.ds(pl.multiple_of(step * LANE, LANE), LANE)
        places, weights = [], []
        for corner in range(4):
            cell = st[corner : corner + 1, lanes] - CW
            cell = jnp.where(cell < 0, cell + span, cell)
            places.append(jnp.broadcast_to(cell, (pack, LANE)).astype(jnp.int16))
            weight = w[corner : corner + 1, lanes].astype(F32)
            weights.append(jnp.broadcast_to(weight, (pack, LANE)).astype(BF16))
        for block in range(span // pack):
            index = base_rows + jnp.int16(block * pack)
            value = jnp.zeros((pack, LANE), BF16)
            for corner in range(4):
                value = jnp.where(places[corner] == index, weights[corner], value)
            matrix[step, block * pack : (block + 1) * pack, :] = value
        return carry

    lax.fori_loop(0, fine // LANE, build, 0)

    factors = vert[...].astype(BF16)
    level_k = lax.broadcasted_iota(jnp.int32, (rows, total_levels), 1)
    level_i = lax.broadcasted_iota(jnp.int32, (rows, total_levels), 0)
    pick = jnp.where(level_k == first + level_i, 1.0, 0.0).astype(BF16)
    forward = jnp.dot(pick, factors, preferred_element_type=F32).astype(BF16)
    backward = lax.dot_general(
        pick, factors, (((1,), (1,)), ((), ())), preferred_element_type=F32
    ).astype(BF16)

    def spread_out(source, height, offset):
        wide = window * height
        lane = lax.broadcasted_iota(jnp.int32, (total_levels, wide), 1) // height
        row = lax.broadcasted_iota(jnp.int32, (total_levels, wide), 0)
        chosen = jnp.where(row == first + offset(lane), 1.0, 0.0).astype(BF16)
        lines = jnp.dot(source, chosen, preferred_element_type=F32)
        at = lax.broadcasted_iota(jnp.int32, (height, wide), 1) % height
        mask = at == lax.broadcasted_iota(jnp.int32, (height, wide), 0)
        return [jnp.where(mask, lines[i : i + 1], 0.0) for i in range(rows)]

    def natural(seg):
        return seg - HB

    def stored(seg):
        return jnp.where(
            seg < HB, seg - HB,
            jnp.where(seg < rows, seg, jnp.where(seg < rows + HB, seg - rows, seg - HB)),
        )

    order = list(range(HB, rows)) + list(range(HB))
    blocks = spread_out(forward, members, natural)
    for place, i in enumerate(order):
        am[place * members : (place + 1) * members, :] = blocks[i].astype(BF16)
    blocks = spread_out(backward, members, stored)
    for i in range(rows):
        bm[i * members : (i + 1) * members, :] = blocks[i].astype(BF16)
    for out, source in ((ac, forward), (bc, backward)):
        blocks = spread_out(source, group, natural)
        for i in range(0, rows, 2):
            both = jnp.concatenate(blocks[i : i + 2], axis=0)
            out[i * group : (i + 2) * group, :] = both.astype(BF16)

    def localize(members_in, coarse_in, coarse_by, out):
        wide = members_in.shape[-1]
        value = jnp.dot(
            am[...], members_in.reshape(window * members, wide), preferred_element_type=F32
        ).astype(BF16)
        out[0:comb_at, :] = value[0:comb_at]
        out[low_at:, :] = value[comb_at:]
        flat = coarse_in.astype(F32).reshape(window * group, wide).astype(BF16)
        local = jnp.dot(ac[...], flat, preferred_element_type=F32).reshape(rows, group, wide)
        out[comb_at:low_at, :] = jnp.sum(local * coarse_by.astype(F32), axis=1).astype(BF16)

    def strip(ref, chunk, r0, r1):
        parts = [ref[chunk * WIDE + i, r0:r1, :] for i in range(WIDE)]
        return jnp.concatenate(parts, axis=1)

    def summed(value, chunk, piece, part):
        lanes = slice(piece * LANE, (piece + 1) * LANE)
        at = (chunk * WIDE + piece) * LANE
        terms, kept = [], []
        for i in range(part * 8, part * 8 + 8):
            member = pert[i, :, at : at + LANE].astype(F32)
            product = member * value[level_at(i) : level_at(i) + members, lanes]
            total = product[0:8]
            for r in range(8, members, 8):
                total = total + product[r : r + 8]
            terms.append(total)
            kept.append(member)
        return fold(terms) + value[comb_at + part * 8 : comb_at + part * 8 + 8, lanes], kept

    when(-1, lambda: settle(filler(near), recv1.at[0]))
    when(1, lambda: settle(filler(near), recv1.at[1]))
    begin(late)
    localize(mc[...], cc[...], cp[own], fld)
    loads[6].wait()
    for chunk in range(fine // (WIDE * LANE)):
        interp = jnp.dot(fld[...], strip(matrix, chunk, 0, cells), preferred_element_type=F32)
        for piece in range(WIDE):
            for part in range(rows // 8):
                total, _ = summed(interp, chunk, piece, part)
                line[chunk * WIDE + piece, part * 8 : part * 8 + 8, :] = total
    def unpack(from_next, from_prev):
        low = lower(from_next.shape)
        nxt, prv = from_next.astype(F32), from_prev.astype(F32)
        return jnp.where(low, nxt, prv), turned(jnp.where(low, prv, nxt))

    def keep(level, value):
        value = value.astype(BF16)
        rim_m[level] = value[0:members]
        rim_c[level] = value[members : members + group]
        if HB <= level < HB + rows:
            rim_p[level - HB] = value[members + group :]

    settle(rt, recv1.at[4])
    for k, (a, b) in enumerate(pairs):
        va, vb = unpack(rt[0, k], rt[1, k])
        keep(HB + a, va)
        keep(HB + b, vb)
    when(-1, lambda: settle(rd.at[0], recv1.at[2]))
    when(1, lambda: settle(rd.at[1], recv1.at[3]))
    for floor in range(2):
        for k in range(half):
            va, vb = unpack(rd[floor, 0, k], rd[floor, 1, k])
            base = floor * (HB + rows)
            keep(base + k, va)
            keep(base + k + half, vb)
    localize(rim_m[...], rim_c[...], rim_p[...], fld_rim)
    for chunk in range(fine // (WIDE * LANE)):
        rim = strip(matrix, chunk, cells, span)
        interp = jnp.dot(fld_rim[...], rim, preferred_element_type=F32)
        for piece in range(WIDE):
            n = chunk * WIDE + piece
            totals = []
            for part in range(rows // 8):
                total, kept = summed(interp, chunk, piece, part)
                total = total + line[n, part * 8 : part * 8 + 8, :]
                totals.append(total)
                for r, member in enumerate(kept):
                    at = level_at(part * 8 + r)
                    adj[n, at : at + members, :] = (member * total[r : r + 1]).astype(BF16)
            adj[n, comb_at:low_at, :] = jnp.concatenate(totals, axis=0).astype(BF16)
        term = lax.dot_general(
            strip(adj, chunk, 0, rows * (members + 1)), rim, (((1,), (1,)), ((), ())),
            preferred_element_type=F32,
        )
        if chunk == 0:
            acc_rim[...] = term
        else:
            acc_rim[...] += term
    def packed_at(k):
        a = pairs[k][0]
        return (k - half) * members if a >= HB else pcomb_at + rows + k * members

    low = lower((members, LANE))
    for k, (a, b) in enumerate(pairs):
        value_a = acc_rim[level_at(a) : level_at(a) + members, :]
        value_b = turned(acc_rim[level_at(b) : level_at(b) + members, :])
        at = slice(packed_at(k), packed_at(k) + members)
        out_rim[1, at, :] = jnp.where(low, value_a, value_b).astype(BF16)
        out_rim[0, at, :] = jnp.where(low, value_b, value_a).astype(BF16)
    for side in range(2):
        out_rim[side, pcomb_at : pcomb_at + rows, :] = acc_rim[comb_at:low_at, :].astype(BF16)

    drain(pk, near + extra + 2 * half * kinds * LANE)
    begin(diag2 + tile2)
    for chunk in range(fine // (DEEP * LANE)):
        taken, met = [], []
        for i in range(DEEP):
            taken.append(adj[chunk * DEEP + i])
            met.append(matrix[chunk * DEEP + i, 0:cells, :])
        term = lax.dot_general(
            jnp.concatenate(taken, axis=1), jnp.concatenate(met, axis=1),
            (((1,), (1,)), ((), ())), preferred_element_type=F32,
        )
        if chunk == 0:
            acc_own[...] = term
        else:
            acc_own[...] += term
    out_own[...] = acc_own[...].astype(BF16)
    begin(lev2)
    when(-1, lambda: settle(filler(extra), recv1.at[5]))
    when(1, lambda: settle(filler(extra), recv1.at[6]))
    settle(r_tile, recv2.at[4])
    for floor, dl in ((0, -1), (1, 1)):
        when(dl, lambda floor=floor: settle(r_diag.at[floor], recv2.at[2 + floor]))
        when(dl, lambda floor=floor: settle(r_lev.at[floor], recv2.at[floor]))
    def zero_but(value, keep_low):
        low = lower(value.shape)
        return jnp.where(low, value, 0.0) if keep_low else jnp.where(low, 0.0, value)

    def joined(base, messages, at, swap):
        from_prev, from_next = messages[1, at, :].astype(F32), messages[0, at, :].astype(F32)
        if swap:
            from_prev, from_next = turned(from_prev), turned(from_next)
        parts = [base[:, i * LANE : (i + 1) * LANE] for i in range(cells // LANE)]
        parts[0] = parts[0] + zero_but(from_prev, True)
        parts[-1] = parts[-1] + zero_but(from_next, False)
        return parts

    def put(ref, r0, rn, parts):
        for i, part in enumerate(parts):
            ref[r0 : r0 + rn, i * LANE : (i + 1) * LANE] = part.astype(BF16)

    def stored_at(i):
        return HB * members + ((i - HB) * members if i >= HB else comb_at + i * members)

    for k, pair in enumerate(pairs):
        at = slice(packed_at(k), packed_at(k) + members)
        for swap, i in enumerate(pair):
            base = acc_own[level_at(i) : level_at(i) + members, :]
            put(xm, stored_at(i), members, joined(base, r_tile, at, swap))
    for floor in range(2):
        p0, o0 = (0, 0) if floor == 0 else (rows, rows)
        x0 = 0 if floor == 0 else HB * members + comb_at + HB * members
        for k in range(half):
            at = slice(p0 + k * members, p0 + (k + 1) * members)
            for swap in range(2):
                i = k + swap * half
                base = r_lev[floor, o0 + i * members : o0 + (i + 1) * members, :].astype(F32)
                put(xm, x0 + i * members, members, joined(base, r_diag.at[floor], at, swap))
    lines = []
    for floor, base in ((0, r_lev), (2, acc_own), (1, r_lev)):
        if floor == 2:
            parts = joined(acc_own[comb_at:low_at, :], r_tile, slice(pcomb_at, pcomb_at + rows), 0)
            chosen = range(rows)
        else:
            o0 = HB * members if floor == 0 else 0
            p0 = HB * members // 2 if floor == 0 else 0
            base = r_lev[floor, o0 : o0 + rows, :].astype(F32)
            parts = joined(base, r_diag.at[floor], slice(p0, p0 + rows), 0)
            chosen = range(rows - HB, rows) if floor == 0 else range(HB)
        lines += [[part[i : i + 1] for part in parts] for i in chosen]
    for level in range(0, window, 2):
        for i in range(cells // LANE):
            lanes = slice(i * LANE, (i + 1) * LANE)
            both = [cp[level + s, :, lanes].astype(F32) * lines[level + s][i] for s in range(2)]
            xc[level * group : (level + 2) * group, lanes] = jnp.concatenate(both, 0).astype(BF16)

    drain(out_rim, edge * cells + 2 * pedge * LANE)


def finish(xm, xc, bm, bc, mo_hbm, co_hbm, mo, co, sem):
    rows, members, cells = mo.shape
    group = co.shape[1]
    step = rows // 2
    copies = []
    for part in range(2):
        levels = pl.ds(part * step, step)
        at = slice(part * step * members, (part + 1) * step * members)
        value = jnp.dot(bm[at, :], xm[...], preferred_element_type=F32)
        mo[levels] = value.reshape(step, members, cells)
        copies.append(pltpu.make_async_copy(mo.at[levels], mo_hbm.at[levels], sem.at[part]))
        copies[-1].start()
    value = jnp.dot(bc[...], xc[...], preferred_element_type=F32)
    co[...] = value.reshape(rows, group, cells)
    copies.append(pltpu.make_async_copy(co, co_hbm, sem.at[2]))
    copies[-1].start()
    for copy in copies:
        copy.wait()


def solution(mesh):
    tiles, levs = mesh.shape["tile"], mesh.shape["lev"]

    def step(members_pert, coarse_pert, member_ctrl, coarse_ctrl, vert_loc, stencil, interp_w):
        rows, members, cells = member_ctrl.shape
        group = coarse_ctrl.shape[1]
        fine = members_pert.shape[2]
        levels, span, lines = rows + 2 * HB, cells + LANE, rows * (members + 1)
        edge = HB * members + rows
        comb_at, packed = dims(rows, members, group, cells)
        pedge = HB * members // 2 + rows
        hbm = pl.BlockSpec(memory_space=pl.ANY)
        kinds = members + 2 * group
        vmem = pl.BlockSpec(memory_space=pltpu.VMEM)
        results = pl.pallas_call(
            functools.partial(kernel, tiles, levs),
            out_shape=(
                pltpu.VMEM((levels * members, cells), BF16),
                pltpu.VMEM((levels * group, cells), BF16),
                pltpu.VMEM((rows * members, levels * members), BF16),
                pltpu.VMEM((rows * group, levels * group), BF16),
            ),
            in_specs=[hbm] * 7,
            out_specs=(vmem,) * 4,
            scratch_shapes=[
                pltpu.VMEM((levels, members, cells), BF16),
                pltpu.VMEM((levels, group, cells), BF16),
                pltpu.VMEM((levels, group, cells), BF16),
                pltpu.VMEM((rows, members, fine), BF16),
                pltpu.VMEM(vert_loc.shape, F32),
                pltpu.VMEM(stencil.shape, jnp.int32),
                pltpu.VMEM(interp_w.shape, BF16),
                pltpu.VMEM((fine // LANE, span, LANE), BF16),
                pltpu.VMEM((rows * members, levels * members), BF16),
                pltpu.VMEM((rows * group, levels * group), BF16),
                pltpu.VMEM((levels, members, LANE), BF16),
                pltpu.VMEM((levels, group, LANE), BF16),
                pltpu.VMEM((rows, group, LANE), BF16),
                pltpu.VMEM((2, rows // 2, kinds, LANE), BF16),
                pltpu.VMEM((2, rows // 2, kinds, LANE), BF16),
                pltpu.VMEM((2, 2, HB // 2, kinds, LANE), BF16),
                pltpu.VMEM((lines, cells), BF16),
                pltpu.VMEM((lines, LANE), BF16),
                pltpu.VMEM((fine // LANE, lines, LANE), BF16),
                pltpu.VMEM((fine // LANE, rows, LANE), F32),
                pltpu.VMEM((lines, LANE), F32),
                pltpu.VMEM((lines, cells), BF16),
                pltpu.VMEM((2, packed, LANE), BF16),
                pltpu.VMEM((lines, cells), F32),
                pltpu.VMEM((2, packed, LANE), BF16),
                pltpu.VMEM((2, edge, cells), BF16),
                pltpu.VMEM((2, 2, pedge, LANE), BF16),
                pltpu.SemaphoreType.DMA((7,)),
                pltpu.SemaphoreType.DMA((3,)),
                pltpu.SemaphoreType.DMA((7,)),
                pltpu.SemaphoreType.DMA((5,)),
            ],
            compiler_params=pltpu.CompilerParams(
                collective_id=0, has_side_effects=True, vmem_limit_bytes=56 * 1024 * 1024
            ),
        )(members_pert, coarse_pert, member_ctrl, coarse_ctrl, vert_loc, stencil, interp_w)
        return pl.pallas_call(
            finish,
            out_shape=(
                jax.ShapeDtypeStruct((rows, members, cells), F32),
                jax.ShapeDtypeStruct((rows, group, cells), F32),
            ),
            in_specs=[vmem] * 4,
            out_specs=(hbm, hbm),
            scratch_shapes=[
                pltpu.VMEM((rows, members, cells), F32),
                pltpu.VMEM((rows, group, cells), F32),
                pltpu.SemaphoreType.DMA((3,)),
            ],
            compiler_params=pltpu.CompilerParams(vmem_limit_bytes=4 * 1024 * 1024),
        )(*results)

    in_specs = (
        P("lev", None, "tile"),
        P("lev", None, "tile"),
        P("lev", None, "tile"),
        P("lev", None, "tile"),
        P(),
        P(None, "tile"),
        P(None, "tile"),
    )
    out_specs = (P("lev", None, "tile"), P("lev", None, "tile"))
    return jax.shard_map(step, mesh=mesh, in_specs=in_specs, out_specs=out_specs, check_vma=False)
```

```python
import functools

import jax
import jax.numpy as jnp
from jax import lax
from jax.experimental import pallas as pl
from jax.experimental.pallas import tpu as pltpu
from jax.sharding import PartitionSpec as P

HB = 4
CW = 64
LANE = 128
WIDE = 2
MESH = pl.DeviceIdType.MESH
F32 = jnp.float32
BF16 = jnp.bfloat16

DIRECTIONS = ((0, -1), (0, 1), (-1, 0), (1, 0), (-1, -1), (1, -1), (-1, 1), (1, 1))


def pairs_of(rows):
    half = HB // 2
    return [(b + k, b + k + half) for b in range(0, rows, HB) for k in range(half)]


def order_of(rows):
    return list(range(rows - HB, rows)) + list(range(HB)) + list(range(HB, rows - HB))


def fold(values):
    row = lax.broadcasted_iota(jnp.int32, (8, LANE), 0)
    for stride in (1, 2, 4):
        even = (row // stride) % 2 == 0
        values = [
            jnp.where(even, a, b) + pltpu.roll(jnp.where(even, b, a), stride, 0)
            for a, b in zip(values[0::2], values[1::2])
        ]
    return values[0]


def kernel(tiles, levs, *refs):
    rows, members, cells = refs[2].shape
    group = refs[3].shape[1]
    whole, coarse, few = rows * (members + 1), rows * group, rows
    scopes = [
        pltpu.ACC(mxu)((height, cells), F32)
        for height in (whole, whole, whole, coarse, few) for mxu in range(2)
    ]
    pl.run_scoped(lambda *sums: body(tiles, levs, sums, *refs), *scopes)


def body(
    tiles, levs, sums, pert_hbm, cp_hbm, mc_hbm, cc_hbm, vert_hbm, st_hbm, w_hbm, xm, xc, bm, bc,
    mc, cc, cp, pert, vert, st, w, matrix, am, ac, rim_m, rim_c, rim_p, pk, rt, rd,
    fld, fld_rim, adj, line, acc_rim, out_own, out_rim, acc_own, r_tile, r_lev, r_diag,
    load_sem, send, recv1, recv2, ready,
):
    rows, members, cells = mc_hbm.shape
    group = cc_hbm.shape[1]
    total_levels = vert_hbm.shape[0]
    fine = pert_hbm.shape[2]
    span = cells + LANE
    window = rows + 2 * HB
    edge = HB * members + rows
    last = cells - LANE
    comb_at, low_at = HB * members, HB * members + rows
    whole = rows * (members + 1)
    pcomb_at = comb_at // 2
    pedge = pcomb_at + rows
    order = order_of(rows)
    pairs = pairs_of(rows)
    half = HB // 2
    kinds = members + 2 * group

    def level_at(i):
        place = order.index(i)
        return place * members + (rows if place >= HB else 0)

    assert cells == WIDE * LANE and window * members <= 2 * cells and window * group <= cells
    ahead, behind, rim_sum, coarse_sum, few_sum = (sums[i : i + 2] for i in range(0, 10, 2))
    turns = [0, 0]

    def product(into, mxu, left, right, transpose=False):
        turn = turns[mxu]
        turns[mxu] = 1 - turn
        pltpu.matmul_push_rhs(right, staging_register=turn, mxu_index=mxu, transpose=transpose)
        pltpu.matmul_acc_lhs(into[mxu], left, load_staged_rhs=turn)

    t = lax.axis_index("tile")
    v = lax.axis_index("lev")
    first = v * rows
    has = {-1: v > 0, 0: None, 1: v < levs - 1}
    beside = {-1: jnp.where(t == 0, tiles - 1, t - 1), 0: t, 1: jnp.where(t == tiles - 1, 0, t + 1)}

    def when(dl, action):
        if dl == 0:
            action()
        else:
            pl.when(has[dl])(action)

    def begin(copies):
        for dl, copy in copies:
            when(dl, copy.start)

    def start_first(copies):
        for dl, copy in copies:
            pl.when(jnp.logical_and(v == 0, levs > 1))(copy.start)

    def settle(ref, sem):
        pltpu.make_async_copy(ref, ref, sem).wait()

    def filler(count):
        return pert.at[0, :, pl.ds(0, count // members)]

    def drain(ref, count):
        settle(ref, send.at[0])
        when(1, lambda: settle(filler(count), send.at[1]))
        when(-1, lambda: settle(filler(count), send.at[2]))

    own = pl.ds(HB, rows)
    loads = [
        pltpu.make_async_copy(mc_hbm, mc.at[own], load_sem.at[0]),
        pltpu.make_async_copy(cc_hbm, cc.at[own], load_sem.at[1]),
        pltpu.make_async_copy(cp_hbm, cp.at[own], load_sem.at[2]),
        pltpu.make_async_copy(st_hbm, st, load_sem.at[3]),
        pltpu.make_async_copy(w_hbm, w, load_sem.at[4]),
        pltpu.make_async_copy(vert_hbm, vert, load_sem.at[5]),
        pltpu.make_async_copy(pert_hbm, pert, load_sem.at[6]),
    ]
    for load in loads[:3]:
        load.start()

    below = {-1: t > 0, 1: t == tiles - 1}

    def signal(sem, dt, dl):
        pl.semaphore_signal(sem, inc=1, device_id=(beside[dt], v + dl), device_id_type=MESH)

    barrier = pltpu.get_barrier_semaphore()
    for dt in (-1, 1):
        pl.when(jnp.logical_not(below[dt]))(lambda dt=dt: signal(barrier, dt, 0))
    for dt in (-1, 0, 1):
        when(1, lambda dt=dt: signal(barrier, dt, 1))
        pl.when(v == 1)(lambda dt=dt: signal(barrier, dt, -1))
    for load in loads[3:]:
        load.start()
    lower_tiles = jnp.where(t > 0, 1, 0) + jnp.where(t == tiles - 1, 1, 0)
    pl.semaphore_wait(barrier, lower_tiles + (3 if levs > 1 else 0))
    for dt in (-1, 1):
        pl.when(below[dt])(lambda dt=dt: signal(ready.at[0], dt, 0))
    for dt in (-1, 0, 1):
        pl.when(v > 1)(lambda dt=dt: signal(ready.at[1], dt, -1))

    def remote(src, dst, send_at, recv_at, dt, dl):
        return dl, pltpu.make_async_remote_copy(
            src_ref=src, dst_ref=dst, send_sem=send_at, recv_sem=recv_at,
            device_id=(beside[dt], v + dl), device_id_type=MESH,
        )

    level_src = {1: rows, -1: HB}
    level_dst = {1: 0, -1: HB + rows}
    entry_src = {1: len(pairs) - half, -1: 0}
    tile_row = {1: 0, -1: pcomb_at}
    lev_row = {1: 0, -1: comb_at}
    lev1, late, tile1, diag1, tile2, diag2, lev2 = [], [], [], [], [], [], []
    for dl in (-1, 1):
        floor = (1 - dl) // 2
        for buf, copies, at in ((mc, lev1, 0), (cc, lev1, 0), (cp, late, 5)):
            copies.append(remote(
                buf.at[pl.ds(level_src[dl], HB)], buf.at[pl.ds(level_dst[dl], HB)],
                send.at[1 + floor], recv1.at[at + floor], 0, dl))
        lev2.append(remote(
            out_own.at[pl.ds(lev_row[dl], edge)], r_lev.at[floor],
            send.at[1 + floor], recv2.at[floor], 0, dl))
        for dt in (-1, 1):
            side = (1 + dt) // 2
            diag1.append(remote(
                pk.at[side, pl.ds(entry_src[dl], half), pl.ds(0, members + group)],
                rd.at[floor, side],
                send.at[1 + floor], recv1.at[2 + floor], dt, dl))
            diag2.append(remote(
                out_rim.at[side, pl.ds(tile_row[dl], pedge)], r_diag.at[floor, side],
                send.at[1 + floor], recv2.at[2 + floor], dt, dl))
    for dt in (-1, 1):
        side = (1 + dt) // 2
        tile1.append(remote(pk.at[side], rt.at[side], send.at[0], recv1.at[4], dt, 0))
        tile2.append(remote(out_rim.at[side], r_tile.at[side], send.at[0], recv2.at[4], dt, 0))
    near = HB * (members + group) * cells
    extra = HB * group * cells

    @pl.when(v == 0)
    def _():
        for buf in (mc, cc, cp):
            buf[0:HB] = jnp.zeros((HB,) + buf.shape[1:], BF16)
        rd[0] = jnp.zeros(rd.shape[1:], BF16)
        r_lev[0] = jnp.zeros(r_lev.shape[1:], BF16)
        r_diag[0] = jnp.zeros(r_diag.shape[1:], BF16)

    @pl.when(v == levs - 1)
    def _():
        for buf in (mc, cc, cp):
            buf[HB + rows :] = jnp.zeros((HB,) + buf.shape[1:], BF16)
        rd[1] = jnp.zeros(rd.shape[1:], BF16)
        r_lev[1] = jnp.zeros(r_lev.shape[1:], BF16)
        r_diag[1] = jnp.zeros(r_diag.shape[1:], BF16)

    def lower(shape):
        return lax.broadcasted_iota(jnp.int32, shape, len(shape) - 1) < CW

    def turned(value):
        return pltpu.roll(value, CW, 1)

    for load in loads[:3]:
        load.wait()
    begin([x for x in lev1 if x[0] < 0])
    start_first([x for x in lev1 if x[0] > 0])
    for k, (a, b) in enumerate(pairs):
        for buf, r0, rn in ((mc, 0, members), (cc, members, group), (cp, members + group, group)):
            low = lower((rn, LANE))
            near_a, near_b = (buf[HB + i, :, 0:LANE].astype(F32) for i in (a, b))
            far_a, far_b = (buf[HB + i, :, last:].astype(F32) for i in (a, b))
            pk[0, k, r0 : r0 + rn, :] = jnp.where(low, near_a, turned(near_b)).astype(BF16)
            pk[1, k, r0 : r0 + rn, :] = jnp.where(low, turned(far_b), far_a).astype(BF16)
    begin([x for x in diag1 if x[0] < 0])
    start_first([x for x in diag1 if x[0] > 0])
    for dt, (dl, copy) in zip((-1, 1), tile1):
        pl.when(below[dt])(copy.start)
    for load in loads[3:6]:
        load.wait()
    pack = 16
    base_rows = lax.broadcasted_iota(jnp.int32, (pack, LANE), 0).astype(jnp.int16)

    def build(step, carry):
        lanes = pl.ds(pl.multiple_of(step * LANE, LANE), LANE)
        places, weights = [], []
        for corner in range(4):
            cell = st[corner : corner + 1, lanes] - CW
            cell = jnp.where(cell < 0, cell + span, cell)
            places.append(jnp.broadcast_to(cell, (pack, LANE)).astype(jnp.int16))
            weight = w[corner : corner + 1, lanes].astype(F32)
            weights.append(jnp.broadcast_to(weight, (pack, LANE)).astype(BF16))
        for block in range(span // pack):
            index = base_rows + jnp.int16(block * pack)
            value = jnp.zeros((pack, LANE), BF16)
            for corner in range(4):
                value = jnp.where(places[corner] == index, weights[corner], value)
            matrix[step, block * pack : (block + 1) * pack, :] = value
        return carry

    steps = fine // LANE
    lax.fori_loop(0, steps // 2, build, 0)
    pl.when(t < tiles - 1)(lambda: pl.semaphore_wait(ready.at[0], 2 - lower_tiles))
    for dt, (dl, copy) in zip((-1, 1), tile1):
        pl.when(jnp.logical_not(below[dt]))(copy.start)
    lax.fori_loop(steps // 2, steps, build, 0)
    inner = jnp.logical_and(v > 0, v < levs - 1)
    pl.when(inner)(lambda: pl.semaphore_wait(ready.at[1], 3))
    for dl, copy in lev1 + diag1:
        if dl > 0:
            pl.when(inner)(copy.start)

    factors = vert[...].astype(BF16)
    factors = jnp.concatenate(
        [factors, jnp.zeros((total_levels, cells - total_levels), BF16)], axis=1)
    factors = jnp.concatenate(
        [factors, jnp.zeros((cells - total_levels, cells), BF16)], axis=0)
    level_k = lax.broadcasted_iota(jnp.int32, (rows, cells), 1)
    level_i = lax.broadcasted_iota(jnp.int32, (rows, cells), 0)
    pick = jnp.where(level_k == first + level_i, 1.0, 0.0).astype(BF16)
    product(few_sum, 0, pick, factors)
    product(few_sum, 1, pick, factors, transpose=True)
    forward = pltpu.matmul_pop(few_sum[0]).astype(BF16)
    backward = pltpu.matmul_pop(few_sum[1]).astype(BF16)

    def spread_out(source, height, offset, mxu, base):
        shape = (total_levels, cells)
        seg = (lax.broadcasted_iota(jnp.int32, shape, 1) + base) // height
        row = lax.broadcasted_iota(jnp.int32, shape, 0)
        hit = jnp.logical_and(row == first + offset(seg), seg < window)
        chosen = jnp.where(hit, 1.0, 0.0).astype(BF16)
        chosen = jnp.concatenate([chosen, jnp.zeros((cells - total_levels, cells), BF16)], axis=0)
        product(few_sum, mxu, source, chosen)
        return pltpu.matmul_pop(few_sum[mxu])

    def blocks_of(lines, height):
        at = lax.broadcasted_iota(jnp.int32, (height, LANE), 1) % height
        mask = at == lax.broadcasted_iota(jnp.int32, (height, LANE), 0)
        return [
            [
                jnp.where(mask, line[i : i + 1, p : p + LANE], 0.0)
                for line in lines for p in range(0, cells, LANE)
            ]
            for i in range(rows)
        ]

    def natural(seg):
        return seg - HB

    def stored(seg):
        inner = jnp.where(seg < 2 * HB, seg + rows - 2 * HB, seg - 2 * HB)
        return jnp.where(jnp.logical_or(seg < HB, seg >= rows + HB), seg - HB, inner)

    lines = [spread_out(forward, members, natural, m, m * cells) for m in range(2)]
    for i, pieces in enumerate(blocks_of(lines, members)):
        for p, piece in enumerate(pieces):
            am[p, level_at(i) : level_at(i) + members, :] = piece.astype(BF16)
    for p in range(am.shape[0]):
        am[p, comb_at:low_at, :] = jnp.zeros((rows, LANE), BF16)
    lines = [spread_out(backward, members, stored, m, m * cells) for m in range(2)]
    for i, pieces in enumerate(blocks_of(lines, members)):
        for p, piece in enumerate(pieces):
            if p * LANE < bm.shape[1]:
                bm[i * members : (i + 1) * members, p * LANE : (p + 1) * LANE] = piece.astype(BF16)
    coarse_lines = [
        [spread_out(source, group, natural, m, 0)] for m, source in enumerate((forward, backward))
    ]
    for out, lines in zip((ac, bc), coarse_lines):
        blocks = blocks_of(lines, group)
        if out is ac:
            blocks = [blocks[i] for i in order]
        for i in range(0, rows, 2):
            for p in range(cells // LANE):
                both = jnp.concatenate([blocks[i][p], blocks[i + 1][p]], axis=0)
                out[p, i * group : (i + 2) * group, :] = both.astype(BF16)

    def side_by_side(ref, p0=0):
        return jnp.concatenate([ref[p0], ref[p0 + 1]], axis=1)

    def square(value):
        height, wide = value.shape
        if wide < cells:
            value = jnp.concatenate([value, jnp.zeros((height, cells - wide), BF16)], axis=1)
        if height < cells:
            value = jnp.concatenate([value, jnp.zeros((cells - height, cells), BF16)], axis=0)
        return value

    def localize(members_in, coarse_in, coarse_by, out):
        wide = members_in.shape[-1]
        flat = members_in.reshape(window * members, wide)
        product(ahead, 0, side_by_side(am), square(flat[0:cells]))
        product(ahead, 1, side_by_side(am, 2), square(flat[cells:]))
        flat = coarse_in.astype(F32).reshape(window * group, wide).astype(BF16)
        product(coarse_sum, 1, side_by_side(ac), square(flat))
        value = pltpu.matmul_pop(ahead[0]) + pltpu.matmul_pop(ahead[1])
        local = pltpu.matmul_pop(coarse_sum[1])
        for p in range(wide // LANE):
            lanes = slice(p * LANE, (p + 1) * LANE)
            part = value[:, lanes].astype(BF16)
            out[p, 0:comb_at, :] = part[0:comb_at]
            out[p, low_at:, :] = part[low_at:]
            mixed = [
                local[place * group : (place + 1) * group, lanes] * coarse_by[i, :, lanes].astype(F32)
                for place, i in enumerate(order)
            ]
            sums = [fold(mixed[g : g + 8]) for g in range(0, rows, 8)]
            out[p, comb_at:low_at, :] = jnp.concatenate(sums, axis=0).astype(BF16)

    def strip(ref, chunk, r0, r1):
        parts = [ref[chunk * WIDE + i, r0:r1, :] for i in range(WIDE)]
        return jnp.concatenate(parts, axis=1)

    def summed(value, chunk, part):
        terms = [[] for _ in range(WIDE)]
        for i in order[part * 8 : part * 8 + 8]:
            for piece in range(WIDE):
                lanes = slice(piece * LANE, (piece + 1) * LANE)
                at = (chunk * WIDE + piece) * LANE
                member = pert[i, :, at : at + LANE].astype(F32)
                product_ = member * value[level_at(i) : level_at(i) + members, lanes]
                total = product_[0:8]
                for r in range(8, members, 8):
                    total = total + product_[r : r + 8]
                terms[piece].append(total)
        at = comb_at + part * 8
        return [
            fold(terms[piece]) + value[at : at + 8, piece * LANE : (piece + 1) * LANE]
            for piece in range(WIDE)
        ]

    when(-1, lambda: settle(filler(near), recv1.at[0]))
    when(1, lambda: settle(filler(near), recv1.at[1]))
    begin(late)
    localize(mc[...], cc[...], cp[own], fld)
    loads[6].wait()
    chunks = fine // (WIDE * LANE)

    def slot(chunk):
        return (ahead, behind)[(chunk // 2) % 2], chunk % 2

    def first_product(chunk):
        product(*slot(chunk), side_by_side(fld), strip(matrix, chunk, 0, cells))

    for chunk in range(min(4, chunks)):
        first_product(chunk)
    for chunk in range(chunks):
        into, mxu = slot(chunk)
        interp = pltpu.matmul_pop(into[mxu])
        if chunk + 4 < chunks:
            first_product(chunk + 4)
        for part in range(rows // 8):
            for piece, total in enumerate(summed(interp, chunk, part)):
                line[chunk * WIDE + piece, part * 8 : part * 8 + 8, :] = total
    def unpack(from_next, from_prev):
        low = lower(from_next.shape)
        nxt, prv = from_next.astype(F32), from_prev.astype(F32)
        return jnp.where(low, nxt, prv), turned(jnp.where(low, prv, nxt))

    def keep(level, value):
        value = value.astype(BF16)
        rim_m[level] = value[0:members]
        rim_c[level] = value[members : members + group]
        if HB <= level < HB + rows:
            rim_p[level - HB] = value[members + group :]

    settle(rt, recv1.at[4])
    for k, (a, b) in enumerate(pairs):
        va, vb = unpack(rt[0, k], rt[1, k])
        keep(HB + a, va)
        keep(HB + b, vb)
    when(-1, lambda: settle(rd.at[0], recv1.at[2]))
    when(1, lambda: settle(rd.at[1], recv1.at[3]))
    for floor in range(2):
        for k in range(half):
            va, vb = unpack(rd[floor, 0, k], rd[floor, 1, k])
            base = floor * (HB + rows)
            keep(base + k, va)
            keep(base + k + half, vb)
    localize(rim_m[...], rim_c[...], rim_p[...], fld_rim)
    rim_fields = jnp.concatenate([fld_rim[0], jnp.zeros((whole, cells - LANE), BF16)], axis=1)
    def rim_of(chunk):
        return square(strip(matrix, chunk, cells, span))

    def rim_product(chunk):
        product(*slot(chunk), rim_fields, rim_of(chunk))

    def own_product(chunk):
        product(
            ahead, chunk % 2, strip(adj, chunk, 0, whole), strip(matrix, chunk, 0, cells),
            transpose=True,
        )

    for chunk in range(min(4, chunks)):
        rim_product(chunk)
    for chunk in range(chunks):
        into, mxu = slot(chunk)
        interp = pltpu.matmul_pop(into[mxu])
        if chunk + 4 < chunks:
            rim_product(chunk + 4)
        totals = [[] for _ in range(WIDE)]
        for part in range(rows // 8):
            for piece, total in enumerate(summed(interp, chunk, part)):
                n = chunk * WIDE + piece
                total = total + line[n, part * 8 : part * 8 + 8, :]
                totals[piece].append(total)
                for r, i in enumerate(order[part * 8 : part * 8 + 8]):
                    by = jnp.broadcast_to(total[r : r + 1], (members, LANE)).astype(BF16)
                    at = level_at(i)
                    lanes = slice(n * LANE, (n + 1) * LANE)
                    adj[n, at : at + members, :] = pert[i, :, lanes] * by
        for piece in range(WIDE):
            both = jnp.concatenate(totals[piece], axis=0)
            adj[chunk * WIDE + piece, comb_at:low_at, :] = both.astype(BF16)
        product(rim_sum, mxu, strip(adj, chunk, 0, whole), rim_of(chunk), transpose=True)
    early = min(4, chunks)
    for chunk in range(early):
        own_product(chunk)
    back = pltpu.matmul_pop(rim_sum[0]) + pltpu.matmul_pop(rim_sum[1])
    acc_rim[...] = back[:, 0:LANE]
    def packed_at(k):
        place = order.index(pairs[k][0])
        entry = place // HB * half + place % HB
        return entry * members + (rows if place >= HB else 0)

    low = lower((members, LANE))
    for k, (a, b) in enumerate(pairs):
        value_a = acc_rim[level_at(a) : level_at(a) + members, :]
        value_b = turned(acc_rim[level_at(b) : level_at(b) + members, :])
        at = slice(packed_at(k), packed_at(k) + members)
        out_rim[1, at, :] = jnp.where(low, value_a, value_b).astype(BF16)
        out_rim[0, at, :] = jnp.where(low, value_b, value_a).astype(BF16)
    for side in range(2):
        out_rim[side, pcomb_at : pcomb_at + rows, :] = acc_rim[comb_at:low_at, :].astype(BF16)

    drain(pk, near + extra + 2 * half * (members + group) * LANE)
    begin(diag2 + tile2)
    for chunk in range(early, chunks):
        own_product(chunk)
    acc_own[...] = pltpu.matmul_pop(ahead[0]) + pltpu.matmul_pop(ahead[1])
    out_own[...] = acc_own[...].astype(BF16)
    begin(lev2)
    when(-1, lambda: settle(filler(extra), recv1.at[5]))
    when(1, lambda: settle(filler(extra), recv1.at[6]))
    settle(r_tile, recv2.at[4])
    for floor, dl in ((0, -1), (1, 1)):
        when(dl, lambda floor=floor: settle(r_diag.at[floor], recv2.at[2 + floor]))
    for floor, dl in ((0, -1), (1, 1)):
        when(dl, lambda floor=floor: settle(r_lev.at[floor], recv2.at[floor]))
    def zero_but(value, keep_low):
        low = lower(value.shape)
        return jnp.where(low, value, 0.0) if keep_low else jnp.where(low, 0.0, value)

    def joined(base, messages, at, swap):
        from_prev, from_next = messages[1, at, :].astype(F32), messages[0, at, :].astype(F32)
        if swap:
            from_prev, from_next = turned(from_prev), turned(from_next)
        parts = [base[:, i * LANE : (i + 1) * LANE] for i in range(cells // LANE)]
        parts[0] = parts[0] + zero_but(from_prev, True)
        parts[-1] = parts[-1] + zero_but(from_next, False)
        return parts

    def put(ref, r0, rn, parts):
        for i, part in enumerate(parts):
            ref[r0 : r0 + rn, i * LANE : (i + 1) * LANE] = part.astype(BF16)

    def stored_at(i):
        return (HB + order.index(i)) * members

    for k, pair in enumerate(pairs):
        at = slice(packed_at(k), packed_at(k) + members)
        for swap, i in enumerate(pair):
            base = acc_own[level_at(i) : level_at(i) + members, :]
            put(xm, stored_at(i), members, joined(base, r_tile, at, swap))
    for floor in range(2):
        p0, o0 = (0, 0) if floor == 0 else (rows, rows)
        x0 = 0 if floor == 0 else (HB + rows) * members
        for k in range(half):
            at = slice(p0 + k * members, p0 + (k + 1) * members)
            for swap in range(2):
                i = k + swap * half
                base = r_lev[floor, o0 + i * members : o0 + (i + 1) * members, :].astype(F32)
                put(xm, x0 + i * members, members, joined(base, r_diag.at[floor], at, swap))
    lines = []
    for floor in (0, 2, 1):
        if floor == 2:
            parts = joined(acc_own[comb_at:low_at, :], r_tile, slice(pcomb_at, pcomb_at + rows), 0)
            chosen = [order.index(i) for i in range(rows)]
        else:
            o0 = comb_at if floor == 0 else 0
            p0 = pcomb_at if floor == 0 else 0
            base = r_lev[floor, o0 : o0 + rows, :].astype(F32)
            parts = joined(base, r_diag.at[floor], slice(p0, p0 + rows), 0)
            chosen = range(HB) if floor == 0 else range(HB, 2 * HB)
        lines += [[part[i : i + 1] for part in parts] for i in chosen]
    for level in range(0, window, 2):
        for i in range(cells // LANE):
            lanes = slice(i * LANE, (i + 1) * LANE)
            both = [cp[level + s, :, lanes].astype(F32) * lines[level + s][i] for s in range(2)]
            xc[level * group : (level + 2) * group, lanes] = jnp.concatenate(both, 0).astype(BF16)

    drain(out_rim, edge * cells + 2 * pedge * LANE)


def finish(xm, xc, bm, bc, mo_hbm, co_hbm, mo, co, sem):
    rows, members, cells = mo.shape
    group = co.shape[1]
    step = rows // 2
    copies = []
    for part in range(2):
        levels = pl.ds(part * step, step)
        at = slice(part * step * members, (part + 1) * step * members)
        value = jnp.dot(bm[at, :], xm[...], preferred_element_type=F32)
        mo[levels] = value.reshape(step, members, cells)
        copies.append(pltpu.make_async_copy(mo.at[levels], mo_hbm.at[levels], sem.at[part]))
        copies[-1].start()
    left = jnp.concatenate([bc[0], bc[1]], axis=1)[:, 0 : xc.shape[0]]
    value = jnp.dot(left, xc[...], preferred_element_type=F32)
    co[...] = value.reshape(rows, group, cells)
    copies.append(pltpu.make_async_copy(co, co_hbm, sem.at[2]))
    copies[-1].start()
    for copy in copies:
        copy.wait()


def solution(mesh):
    tiles, levs = mesh.shape["tile"], mesh.shape["lev"]

    def step(members_pert, coarse_pert, member_ctrl, coarse_ctrl, vert_loc, stencil, interp_w):
        rows, members, cells = member_ctrl.shape
        group = coarse_ctrl.shape[1]
        fine = members_pert.shape[2]
        levels, span, lines = rows + 2 * HB, cells + LANE, rows * (members + 1)
        edge = HB * members + rows
        pedge = HB * members // 2 + rows
        packed = rows * members // 2 + rows
        hbm = pl.BlockSpec(memory_space=pl.ANY)
        kinds = members + 2 * group
        vmem = pl.BlockSpec(memory_space=pltpu.VMEM)
        results = pl.pallas_call(
            functools.partial(kernel, tiles, levs),
            out_shape=(
                pltpu.VMEM((levels * members, cells), BF16),
                pltpu.VMEM((levels * group, cells), BF16),
                pltpu.VMEM((rows * members, levels * members), BF16),
                pltpu.VMEM((cells // LANE, rows * group, LANE), BF16),
            ),
            in_specs=[hbm] * 7,
            out_specs=(vmem,) * 4,
            scratch_shapes=[
                pltpu.VMEM((levels, members, cells), BF16),
                pltpu.VMEM((levels, group, cells), BF16),
                pltpu.VMEM((levels, group, cells), BF16),
                pltpu.VMEM((rows, members, fine), BF16),
                pltpu.VMEM(vert_loc.shape, F32),
                pltpu.VMEM(stencil.shape, jnp.int32),
                pltpu.VMEM(interp_w.shape, BF16),
                pltpu.VMEM((fine // LANE, span, LANE), BF16),
                pltpu.VMEM((2 * cells // LANE, lines, LANE), BF16),
                pltpu.VMEM((cells // LANE, rows * group, LANE), BF16),
                pltpu.VMEM((levels, members, LANE), BF16),
                pltpu.VMEM((levels, group, LANE), BF16),
                pltpu.VMEM((rows, group, LANE), BF16),
                pltpu.VMEM((2, rows // 2, kinds, LANE), BF16),
                pltpu.VMEM((2, rows // 2, kinds, LANE), BF16),
                pltpu.VMEM((2, 2, HB // 2, members + group, LANE), BF16),
                pltpu.VMEM((cells // LANE, lines, LANE), BF16),
                pltpu.VMEM((1, lines, LANE), BF16),
                pltpu.VMEM((fine // LANE, lines, LANE), BF16),
                pltpu.VMEM((fine // LANE, rows, LANE), F32),
                pltpu.VMEM((lines, LANE), F32),
                pltpu.VMEM((lines, cells), BF16),
                pltpu.VMEM((2, packed, LANE), BF16),
                pltpu.VMEM((lines, cells), F32),
                pltpu.VMEM((2, packed, LANE), BF16),
                pltpu.VMEM((2, edge, cells), BF16),
                pltpu.VMEM((2, 2, pedge, LANE), BF16),
                pltpu.SemaphoreType.DMA((7,)),
                pltpu.SemaphoreType.DMA((3,)),
                pltpu.SemaphoreType.DMA((7,)),
                pltpu.SemaphoreType.DMA((5,)),
                pltpu.SemaphoreType.REGULAR((2,)),
            ],
            compiler_params=pltpu.CompilerParams(
                collective_id=0, has_side_effects=True, vmem_limit_bytes=56 * 1024 * 1024
            ),
        )(members_pert, coarse_pert, member_ctrl, coarse_ctrl, vert_loc, stencil, interp_w)
        return pl.pallas_call(
            finish,
            out_shape=(
                jax.ShapeDtypeStruct((rows, members, cells), F32),
                jax.ShapeDtypeStruct((rows, group, cells), F32),
            ),
            in_specs=[vmem] * 4,
            out_specs=(hbm, hbm),
            scratch_shapes=[
                pltpu.VMEM((rows, members, cells), F32),
                pltpu.VMEM((rows, group, cells), F32),
                pltpu.SemaphoreType.DMA((3,)),
            ],
            compiler_params=pltpu.CompilerParams(vmem_limit_bytes=4 * 1024 * 1024),
        )(*results)

    in_specs = (
        P("lev", None, "tile"),
        P("lev", None, "tile"),
        P("lev", None, "tile"),
        P("lev", None, "tile"),
        P(),
        P(None, "tile"),
        P(None, "tile"),
    )
    out_specs = (P("lev", None, "tile"), P("lev", None, "tile"))
    return jax.shard_map(step, mesh=mesh, in_specs=in_specs, out_specs=out_specs, check_vma=False)
```

```python
import functools

import jax
import jax.numpy as jnp
from jax import lax
from jax.experimental import pallas as pl
from jax.experimental.pallas import tpu as pltpu
from jax.sharding import PartitionSpec as P

HB = 4
CW = 64
LANE = 128
WIDE = 2
MESH = pl.DeviceIdType.MESH
F32 = jnp.float32
BF16 = jnp.bfloat16

DIRECTIONS = ((0, -1), (0, 1), (-1, 0), (1, 0), (-1, -1), (1, -1), (-1, 1), (1, 1))


def pairs_of(rows):
    half = HB // 2
    return [(b + k, b + k + half) for b in range(0, rows, HB) for k in range(half)]


def order_of(rows):
    return list(range(rows - HB, rows)) + list(range(HB)) + list(range(HB, rows - HB))


def fold(values):
    row = lax.broadcasted_iota(jnp.int32, (8, LANE), 0)
    for stride in (1, 2, 4):
        even = (row // stride) % 2 == 0
        values = [
            jnp.where(even, a, b) + pltpu.roll(jnp.where(even, b, a), stride, 0)
            for a, b in zip(values[0::2], values[1::2])
        ]
    return values[0]


def kernel(tiles, levs, *refs):
    rows, members, cells = refs[2].shape
    group = refs[3].shape[1]
    outer, inner = 2 * HB * members + rows, (rows - 2 * HB) * members
    heights = (outer, inner, outer, inner, outer + inner, outer, rows)
    scopes = [pltpu.ACC(mxu)((height, cells), F32) for height in heights for mxu in range(2)]
    pl.run_scoped(lambda *sums: body(tiles, levs, sums, *refs), *scopes)


def body(
    tiles, levs, sums, pert_hbm, cp_hbm, mc_hbm, cc_hbm, vert_hbm, st_hbm, w_hbm, xm, xc, bm, bc,
    mc, cc, cp, pert, vert, st, w, matrix, am, ac, rim_m, rim_c, rim_p, pk, rt, rd,
    fld, fld_rim, adj, line, acc_rim, out_own, out_rim, acc_own, r_tile, r_lev, r_diag,
    load_sem, send, recv1, recv2, ready,
):
    rows, members, cells = mc_hbm.shape
    group = cc_hbm.shape[1]
    total_levels = vert_hbm.shape[0]
    fine = pert_hbm.shape[2]
    span = cells + LANE
    window = rows + 2 * HB
    edge = HB * members + 2 * HB
    last = cells - LANE
    comb_at, low_at = HB * members, HB * members + rows
    whole = rows * (members + 1)
    pcomb_at = comb_at // 2
    pedge = pcomb_at + 2 * HB
    pinner_at = rows * members // 2 + 2 * HB
    order = order_of(rows)
    pairs = pairs_of(rows)
    half = HB // 2
    kinds = members + 2 * group

    def level_at(i):
        place = order.index(i)
        return place * members + (rows if place >= HB else 0)

    assert cells == WIDE * LANE and window * members <= 2 * cells and window * group <= cells
    slots = [(sums[i : i + 2], sums[i + 2 : i + 4]) for i in (0, 4)]
    rim_sum, half_sum, few_sum = (sums[i : i + 2] for i in (8, 10, 12))
    outer, inner = 2 * HB * members + rows, (rows - 2 * HB) * members
    assert inner == rows * group
    turns = [0, 0]

    def product(into, mxu, left, right, transpose=False):
        turn = turns[mxu]
        turns[mxu] = 1 - turn
        pltpu.matmul_push_rhs(right, staging_register=turn, mxu_index=mxu, transpose=transpose)
        pltpu.matmul_acc_lhs(into[mxu], left, load_staged_rhs=turn)

    def again(into, mxu, left):
        pltpu.matmul_acc_lhs(into[mxu], left)

    t = lax.axis_index("tile")
    v = lax.axis_index("lev")
    first = v * rows
    has = {-1: v > 0, 0: None, 1: v < levs - 1}
    beside = {-1: jnp.where(t == 0, tiles - 1, t - 1), 0: t, 1: jnp.where(t == tiles - 1, 0, t + 1)}

    def when(dl, action):
        if dl == 0:
            action()
        else:
            pl.when(has[dl])(action)

    def begin(copies):
        for dl, copy in copies:
            when(dl, copy.start)

    def start_first(copies):
        for dl, copy in copies:
            pl.when(jnp.logical_and(v == 0, levs > 1))(copy.start)

    def settle(ref, sem):
        pltpu.make_async_copy(ref, ref, sem).wait()

    def filler(count):
        return pert.at[0, :, pl.ds(0, count // members)]

    def drain(ref, count):
        settle(ref, send.at[0])
        when(1, lambda: settle(filler(count), send.at[1]))
        when(-1, lambda: settle(filler(count), send.at[2]))

    own = pl.ds(0, rows)
    loads = [
        pltpu.make_async_copy(mc_hbm, mc.at[own], load_sem.at[0]),
        pltpu.make_async_copy(cc_hbm, cc.at[own], load_sem.at[1]),
        pltpu.make_async_copy(cp_hbm, cp.at[own], load_sem.at[2]),
        pltpu.make_async_copy(st_hbm, st, load_sem.at[3]),
        pltpu.make_async_copy(w_hbm, w, load_sem.at[4]),
        pltpu.make_async_copy(vert_hbm, vert, load_sem.at[5]),
        pltpu.make_async_copy(pert_hbm, pert, load_sem.at[6]),
    ]
    for load in loads[:3]:
        load.start()

    below = {-1: t > 0, 1: t == tiles - 1}

    def signal(sem, dt, dl):
        pl.semaphore_signal(sem, inc=1, device_id=(beside[dt], v + dl), device_id_type=MESH)

    barrier = pltpu.get_barrier_semaphore()
    for dt in (-1, 1):
        greets = jnp.logical_or(v <= 1, jnp.logical_not(below[dt]))
        pl.when(greets)(lambda dt=dt: signal(barrier, dt, 0))
    for dt in (-1, 0, 1):
        when(1, lambda dt=dt: signal(barrier, dt, 1))
        pl.when(v == 1)(lambda dt=dt: signal(barrier, dt, -1))
    for load in loads[3:]:
        load.start()
    pack = 16
    base_rows = lax.broadcasted_iota(jnp.int32, (pack, LANE), 0).astype(jnp.int16)

    def build(step, carry):
        lanes = pl.ds(pl.multiple_of(step * LANE, LANE), LANE)
        places, weights = [], []
        for corner in range(4):
            cell = st[corner : corner + 1, lanes] - CW
            cell = jnp.where(cell < 0, cell + span, cell)
            places.append(jnp.broadcast_to(cell, (pack, LANE)).astype(jnp.int16))
            weight = w[corner : corner + 1, lanes].astype(F32)
            weights.append(jnp.broadcast_to(weight, (pack, LANE)).astype(BF16))
        for block in range(span // pack):
            index = base_rows + jnp.int16(block * pack)
            value = jnp.zeros((pack, LANE), BF16)
            for corner in range(4):
                value = jnp.where(places[corner] == index, weights[corner], value)
            matrix[step, block * pack : (block + 1) * pack, :] = value
        return carry

    steps = fine // LANE

    def build_part(begin_at, end_at):
        if begin_at == 0:
            for load in loads[3:6]:
                load.wait()
        lax.fori_loop(begin_at, end_at, build, 0)

    pl.when(v == 0)(lambda: build_part(0, steps // 2))
    lower_tiles = jnp.where(t > 0, 1, 0) + jnp.where(t == tiles - 1, 1, 0)
    greeting = jnp.where(v <= 1, 2, lower_tiles)
    pl.semaphore_wait(barrier, greeting + (3 if levs > 1 else 0))
    for dt in (-1, 1):
        answers = jnp.logical_and(v > 1, below[dt])
        pl.when(answers)(lambda dt=dt: signal(ready.at[0], dt, 0))
    for dt in (-1, 0, 1):
        pl.when(v > 1)(lambda dt=dt: signal(ready.at[1], dt, -1))

    def remote(src, dst, send_at, recv_at, dt, dl):
        return dl, pltpu.make_async_remote_copy(
            src_ref=src, dst_ref=dst, send_sem=send_at, recv_sem=recv_at,
            device_id=(beside[dt], v + dl), device_id_type=MESH,
        )

    level_src = {1: rows - HB, -1: 0}
    level_dst = {1: rows, -1: rows + HB}
    entry_src = {1: len(pairs) - half, -1: 0}
    tile_row = {1: 0, -1: pcomb_at}
    lev_row = {1: 0, -1: comb_at}
    lev1, late, tile1, diag1, tile2, diag2, lev2 = [], [], [], [], [], [], []
    for dl in (-1, 1):
        floor = (1 - dl) // 2
        for buf, copies, at in ((mc, lev1, 0), (cc, lev1, 0), (cp, late, None)):
            copies.append(remote(
                buf.at[pl.ds(level_src[dl], HB)], buf.at[pl.ds(level_dst[dl], HB)],
                send.at[1 + floor], recv2.at[floor] if at is None else recv1.at[at + floor], 0, dl))
        lev2.append(remote(
            out_own.at[pl.ds(lev_row[dl], edge)], r_lev.at[floor],
            send.at[1 + floor], recv2.at[floor], 0, dl))
        for dt in (-1, 1):
            side = (1 + dt) // 2
            diag1.append(remote(
                pk.at[side, pl.ds(entry_src[dl], half), pl.ds(0, members + group)],
                rd.at[floor, side],
                send.at[1 + floor], recv1.at[2 + floor], dt, dl))
            diag2.append(remote(
                out_rim.at[side, pl.ds(tile_row[dl], pedge)], r_diag.at[floor, side],
                send.at[1 + floor], recv2.at[floor], dt, dl))
    for dt in (-1, 1):
        side = (1 + dt) // 2
        tile1.append(remote(pk.at[side], rt.at[side], send.at[0], recv1.at[4], dt, 0))
        tile2.append(remote(out_rim.at[side], r_tile.at[side], send.at[0], recv2.at[2], dt, 0))
    near = HB * (members + group) * cells
    extra = HB * group * cells

    @pl.when(v == 0)
    def _():
        for buf in (mc, cc, cp):
            buf[rows : rows + HB] = jnp.zeros((HB,) + buf.shape[1:], BF16)
        rd[0] = jnp.zeros(rd.shape[1:], BF16)
        r_lev[0] = jnp.zeros(r_lev.shape[1:], BF16)
        r_diag[0] = jnp.zeros(r_diag.shape[1:], BF16)

    @pl.when(v == levs - 1)
    def _():
        for buf in (mc, cc, cp):
            buf[rows + HB :] = jnp.zeros((HB,) + buf.shape[1:], BF16)
        rd[1] = jnp.zeros(rd.shape[1:], BF16)
        r_lev[1] = jnp.zeros(r_lev.shape[1:], BF16)
        r_diag[1] = jnp.zeros(r_diag.shape[1:], BF16)

    def lower(shape):
        return lax.broadcasted_iota(jnp.int32, shape, len(shape) - 1) < CW

    def turned(value):
        return pltpu.roll(value, CW, 1)

    for load in loads[:3]:
        load.wait()
    begin([x for x in lev1 if x[0] < 0])
    start_first([x for x in lev1 if x[0] > 0])
    for k, (a, b) in enumerate(pairs):
        for buf, r0, rn in ((mc, 0, members), (cc, members, group), (cp, members + group, group)):
            low = lower((rn, LANE))
            near_a, near_b = (buf[i, :, 0:LANE].astype(F32) for i in (a, b))
            far_a, far_b = (buf[i, :, last:].astype(F32) for i in (a, b))
            pk[0, k, r0 : r0 + rn, :] = jnp.where(low, near_a, turned(near_b)).astype(BF16)
            pk[1, k, r0 : r0 + rn, :] = jnp.where(low, turned(far_b), far_a).astype(BF16)
    begin([x for x in diag1 if x[0] < 0])
    start_first([x for x in diag1 if x[0] > 0])
    for dt, (dl, copy) in zip((-1, 1), tile1):
        pl.when(jnp.logical_or(v <= 1, below[dt]))(copy.start)
    pl.when(v > 0)(lambda: build_part(0, steps // 2))
    asks = jnp.logical_and(v > 1, t < tiles - 1)
    pl.when(asks)(lambda: pl.semaphore_wait(ready.at[0], 2 - lower_tiles))
    for dt, (dl, copy) in zip((-1, 1), tile1):
        pl.when(jnp.logical_and(v > 1, jnp.logical_not(below[dt])))(copy.start)
    build_part(steps // 2, steps)
    factors = vert[...].astype(BF16)
    factors = jnp.concatenate(
        [factors, jnp.zeros((total_levels, cells - total_levels), BF16)], axis=1)
    factors = jnp.concatenate(
        [factors, jnp.zeros((cells - total_levels, cells), BF16)], axis=0)
    level_k = lax.broadcasted_iota(jnp.int32, (rows, cells), 1)
    level_i = lax.broadcasted_iota(jnp.int32, (rows, cells), 0)
    pick = jnp.where(level_k == first + level_i, 1.0, 0.0).astype(BF16)
    product(few_sum, 0, pick, factors)
    product(few_sum, 1, pick, factors, transpose=True)
    forward = pltpu.matmul_pop(few_sum[0]).astype(BF16)
    backward = pltpu.matmul_pop(few_sum[1]).astype(BF16)

    def spread_out(source, height, offset, mxu, base):
        shape = (total_levels, cells)
        seg = (lax.broadcasted_iota(jnp.int32, shape, 1) + base) // height
        row = lax.broadcasted_iota(jnp.int32, shape, 0)
        hit = jnp.logical_and(row == first + offset(seg), seg < window)
        chosen = jnp.where(hit, 1.0, 0.0).astype(BF16)
        chosen = jnp.concatenate([chosen, jnp.zeros((cells - total_levels, cells), BF16)], axis=0)
        product(few_sum, mxu, source, chosen)
        return pltpu.matmul_pop(few_sum[mxu])

    def blocks_of(lines, height):
        at = lax.broadcasted_iota(jnp.int32, (height, LANE), 1) % height
        mask = at == lax.broadcasted_iota(jnp.int32, (height, LANE), 0)
        return [
            [
                jnp.where(mask, line[i : i + 1, p : p + LANE], 0.0)
                for line in lines for p in range(0, cells, LANE)
            ]
            for i in range(rows)
        ]

    def natural(seg):
        halo = jnp.where(seg < rows + HB, seg - rows - HB, seg - HB)
        return jnp.where(seg < rows, seg, halo)

    def stored(seg):
        inner = jnp.where(seg < 2 * HB, seg + rows - 2 * HB, seg - 2 * HB)
        return jnp.where(jnp.logical_or(seg < HB, seg >= rows + HB), seg - HB, inner)

    lines = [spread_out(forward, members, natural, m, m * cells) for m in range(2)]
    for i, pieces in enumerate(blocks_of(lines, members)):
        for p, piece in enumerate(pieces):
            am[p, level_at(i) : level_at(i) + members, :] = piece.astype(BF16)
    for p in range(am.shape[0]):
        am[p, comb_at:low_at, :] = jnp.zeros((rows, LANE), BF16)
    lines = [spread_out(backward, members, stored, m, m * cells) for m in range(2)]
    for i, pieces in enumerate(blocks_of(lines, members)):
        for p, piece in enumerate(pieces):
            if p * LANE < bm.shape[1]:
                bm[i * members : (i + 1) * members, p * LANE : (p + 1) * LANE] = piece.astype(BF16)
    coarse_lines = [
        [spread_out(source, group, natural, m, 0)] for m, source in enumerate((forward, backward))
    ]
    for out, lines in zip((ac, bc), coarse_lines):
        blocks = blocks_of(lines, group)
        if out is ac:
            blocks = [blocks[i] for i in order]
        for i in range(0, rows, 2):
            for p in range(cells // LANE):
                both = jnp.concatenate([blocks[i][p], blocks[i + 1][p]], axis=0)
                out[p, i * group : (i + 2) * group, :] = both.astype(BF16)

    def side_by_side(ref, p0=0):
        return jnp.concatenate([ref[p0], ref[p0 + 1]], axis=1)

    def square(value):
        height, wide = value.shape
        if wide < cells:
            value = jnp.concatenate([value, jnp.zeros((height, cells - wide), BF16)], axis=1)
        if height < cells:
            value = jnp.concatenate([value, jnp.zeros((cells - height, cells), BF16)], axis=0)
        return value

    def banded(r0, r1, p0):
        return jnp.concatenate([am[p0, r0:r1, :], am[p0 + 1, r0:r1, :]], axis=1)

    def flat_of(ref, l0, l1):
        value = ref[l0:l1]
        return square(value.reshape((l1 - l0) * members, value.shape[-1]))

    def coarse_product(into, ref):
        value = ref[...].astype(F32)
        flat = value.reshape(window * group, value.shape[-1]).astype(BF16)
        product(into, 1, side_by_side(ac), square(flat))

    def put_outer(value, local, by_ref, out, wide):
        for p in range(wide // LANE):
            lanes = slice(p * LANE, (p + 1) * LANE)
            part = value[:, lanes].astype(BF16)
            out[p, 0:comb_at, :] = part[0:comb_at]
            out[p, low_at:outer, :] = part[low_at:]
            mixed = [
                local[place * group : (place + 1) * group, lanes] * by_ref[i, :, lanes].astype(F32)
                for place, i in enumerate(order)
            ]
            sums = [fold(mixed[g : g + 8]) for g in range(0, rows, 8)]
            out[p, comb_at:low_at, :] = jnp.concatenate(sums, axis=0).astype(BF16)

    def put_inner(value, out, wide):
        for p in range(wide // LANE):
            out[p, outer:, :] = value[:, p * LANE : (p + 1) * LANE].astype(BF16)

    def strip(ref, chunk, r0, r1):
        parts = [ref[chunk * WIDE + i, r0:r1, :] for i in range(WIDE)]
        return jnp.concatenate(parts, axis=1)

    def summed(value, chunk, part):
        terms = [[] for _ in range(WIDE)]
        for i in order[part * 8 : part * 8 + 8]:
            at = level_at(i) - (outer if part else 0)
            for piece in range(WIDE):
                lanes = slice(piece * LANE, (piece + 1) * LANE)
                fine_at = (chunk * WIDE + piece) * LANE
                member = pert[i, :, fine_at : fine_at + LANE].astype(F32)
                product_ = member * value[at : at + members, lanes]
                total = product_[0:8]
                for r in range(8, members, 8):
                    total = total + product_[r : r + 8]
                terms[piece].append(total)
        return [fold(term) for term in terms]

    def combined(value, piece, part):
        at = comb_at + part * 8
        return value[at : at + 8, piece * LANE : (piece + 1) * LANE]

    chunks = fine // (WIDE * LANE)

    def slot(chunk):
        return slots[(chunk // 2) % 2], chunk % 2

    def sweep(start, take, c0, c1):
        for chunk in range(c0, min(c0 + 4, c1)):
            start(chunk)
        for chunk in range(c0, c1):
            take(chunk, chunk + 4 < c1)

    def begin_inner(chunk):
        into, mxu = slot(chunk)
        product(into[1], mxu, side_by_side(fld)[outer:], strip(matrix, chunk, 0, cells))

    def take_inner(chunk, more):
        into, mxu = slot(chunk)
        value = pltpu.matmul_pop(into[1][mxu])
        if more:
            begin_inner(chunk + 4)
        for piece, total in enumerate(summed(value, chunk, 1)):
            line[chunk * WIDE + piece, 8:16, :] = total

    def begin_outer(chunk):
        into, mxu = slot(chunk)
        product(into[0], mxu, side_by_side(fld)[0:outer], strip(matrix, chunk, 0, cells))

    def take_outer(chunk, more):
        into, mxu = slot(chunk)
        value = pltpu.matmul_pop(into[0][mxu])
        if more:
            begin_outer(chunk + 4)
        for piece, total in enumerate(summed(value, chunk, 0)):
            n = chunk * WIDE + piece
            line[n, 0:8, :] = total + combined(value, piece, 0)
            line[n, 8:16, :] += combined(value, piece, 1)

    inner = jnp.logical_and(v > 0, v < levs - 1)
    pl.when(inner)(lambda: pl.semaphore_wait(ready.at[1], 3))
    for dl, copy in lev1 + diag1:
        if dl > 0:
            pl.when(inner)(copy.start)

    product(slots[0][1], 0, banded(outer, whole, 0), flat_of(mc, 0, rows))
    put_inner(pltpu.matmul_pop(slots[0][1][0]), fld, cells)
    loads[6].wait()
    sweep(begin_inner, take_inner, 0, chunks)
    when(-1, lambda: settle(filler(near), recv1.at[0]))
    when(1, lambda: settle(filler(near), recv1.at[1]))
    begin(late)
    (first_outer, first_inner), _ = slots
    product(first_outer, 0, banded(0, outer, 0), flat_of(mc, 0, rows))
    product(first_outer, 1, banded(0, outer, 2), flat_of(mc, rows, window))
    coarse_product(first_inner, cc)
    value = pltpu.matmul_pop(first_outer[0]) + pltpu.matmul_pop(first_outer[1])
    put_outer(value, pltpu.matmul_pop(first_inner[1]), cp, fld, cells)
    sweep(begin_outer, take_outer, 0, chunks)
    def unpack(from_next, from_prev):
        low = lower(from_next.shape)
        nxt, prv = from_next.astype(F32), from_prev.astype(F32)
        return jnp.where(low, nxt, prv), turned(jnp.where(low, prv, nxt))

    def keep(level, value):
        value = value.astype(BF16)
        rim_m[level] = value[0:members]
        rim_c[level] = value[members : members + group]
        if level < rows:
            rim_p[level] = value[members + group :]

    settle(rt, recv1.at[4])
    for k, (a, b) in enumerate(pairs):
        va, vb = unpack(rt[0, k], rt[1, k])
        keep(a, va)
        keep(b, vb)
    product(half_sum, 0, banded(0, outer, 0), flat_of(rim_m, 0, rows))
    again(first_inner, 0, banded(outer, whole, 0))
    when(-1, lambda: settle(rd.at[0], recv1.at[2]))
    when(1, lambda: settle(rd.at[1], recv1.at[3]))
    for floor in range(2):
        for k in range(half):
            va, vb = unpack(rd[floor, 0, k], rd[floor, 1, k])
            base = rows + floor * HB
            keep(base + k, va)
            keep(base + k + half, vb)
    product(half_sum, 1, banded(0, outer, 2), flat_of(rim_m, rows, window))
    coarse_product(first_inner, rim_c)
    value = pltpu.matmul_pop(half_sum[0]) + pltpu.matmul_pop(half_sum[1])
    put_inner(pltpu.matmul_pop(first_inner[0]), fld_rim, LANE)
    put_outer(value, pltpu.matmul_pop(first_inner[1]), rim_p, fld_rim, LANE)
    rim_fields = jnp.concatenate([fld_rim[0], jnp.zeros((whole, cells - LANE), BF16)], axis=1)
    def rim_of(chunk):
        return square(strip(matrix, chunk, cells, span))

    def begin_rim(chunk):
        into, mxu = slot(chunk)
        product(into[0], mxu, rim_fields[0:outer], rim_of(chunk))
        again(into[1], mxu, rim_fields[outer:])

    def rim_and_first(chunk):
        value = [strip(matrix, chunk, cells, span), strip(matrix, chunk, 0, LANE)]
        return jnp.concatenate(value, axis=0)

    def second_half(chunk):
        return square(strip(matrix, chunk, LANE, cells))

    def take_rim(chunk, more):
        into, mxu = slot(chunk)
        values = [pltpu.matmul_pop(into[part][mxu]) for part in range(2)]
        if more:
            begin_rim(chunk + 4)
        totals = [[] for _ in range(WIDE)]
        for part in range(2):
            for piece, total in enumerate(summed(values[part], chunk, part)):
                n = chunk * WIDE + piece
                total = total + combined(values[0], piece, part)
                total = total + line[n, part * 8 : part * 8 + 8, :]
                totals[piece].append(total)
                for r, i in enumerate(order[part * 8 : part * 8 + 8]):
                    by = jnp.broadcast_to(total[r : r + 1], (members, LANE)).astype(BF16)
                    at = level_at(i)
                    lanes = slice(n * LANE, (n + 1) * LANE)
                    adj[n, at : at + members, :] = pert[i, :, lanes] * by
        for piece in range(WIDE):
            both = jnp.concatenate(totals[piece], axis=0)
            adj[chunk * WIDE + piece, comb_at:low_at, :] = both.astype(BF16)
        product(rim_sum, mxu, strip(adj, chunk, 0, whole), rim_and_first(chunk), transpose=True)
        product(half_sum, mxu, strip(adj, chunk, 0, outer), second_half(chunk), transpose=True)

    sweep(begin_rim, take_rim, 0, chunks)
    back = pltpu.matmul_pop(rim_sum[0]) + pltpu.matmul_pop(rim_sum[1])
    acc_rim[...] = back[:, 0:LANE]
    acc_own[:, 0:LANE] = back[:, LANE:]
    back = pltpu.matmul_pop(half_sum[0]) + pltpu.matmul_pop(half_sum[1])
    acc_own[0:outer, LANE:] = back[:, 0:LANE]
    out_own[0:edge, :] = acc_own[0:edge, :].astype(BF16)
    out_own[edge:, :] = acc_own[low_at:outer, :].astype(BF16)
    def packed_at(k):
        place = order.index(pairs[k][0])
        entry = place // HB * half + place % HB
        return entry * members + (2 * HB if place >= HB else 0)

    low = lower((members, LANE))
    for k, (a, b) in enumerate(pairs):
        value_a = acc_rim[level_at(a) : level_at(a) + members, :]
        value_b = turned(acc_rim[level_at(b) : level_at(b) + members, :])
        at = slice(packed_at(k), packed_at(k) + members)
        out_rim[1, at, :] = jnp.where(low, value_a, value_b).astype(BF16)
        out_rim[0, at, :] = jnp.where(low, value_b, value_a).astype(BF16)
    for side in range(2):
        both = acc_rim[comb_at:low_at, :].astype(BF16)
        out_rim[side, pcomb_at : pcomb_at + 2 * HB, :] = both[0 : 2 * HB]
        out_rim[side, pinner_at:, :] = both[2 * HB :]

    drain(pk, near + extra + 2 * half * (members + group) * LANE)
    begin([x for x in diag2 + lev2 if x[0] < 0] + tile2)
    for chunk in range(chunks):
        part = strip(adj, chunk, outer, whole)
        product(first_inner, chunk % 2, part, second_half(chunk), transpose=True)
    back = pltpu.matmul_pop(first_inner[0]) + pltpu.matmul_pop(first_inner[1])
    acc_own[outer:, LANE:] = back[:, 0:LANE]
    begin([x for x in diag2 + lev2 if x[0] > 0])
    settle(r_tile, recv2.at[2])
    far = extra + edge * cells + 2 * pedge * LANE
    when(-1, lambda: settle(filler(far), recv2.at[0]))
    when(1, lambda: settle(filler(far), recv2.at[1]))
    def zero_but(value, keep_low):
        low = lower(value.shape)
        return jnp.where(low, value, 0.0) if keep_low else jnp.where(low, 0.0, value)

    def joined(base, messages, at, swap):
        from_prev, from_next = messages[1, at, :].astype(F32), messages[0, at, :].astype(F32)
        if swap:
            from_prev, from_next = turned(from_prev), turned(from_next)
        parts = [base[:, i * LANE : (i + 1) * LANE] for i in range(cells // LANE)]
        parts[0] = parts[0] + zero_but(from_prev, True)
        parts[-1] = parts[-1] + zero_but(from_next, False)
        return parts

    def put(ref, r0, rn, parts):
        for i, part in enumerate(parts):
            ref[r0 : r0 + rn, i * LANE : (i + 1) * LANE] = part.astype(BF16)

    def stored_at(i):
        return (HB + order.index(i)) * members

    for k, pair in enumerate(pairs):
        at = slice(packed_at(k), packed_at(k) + members)
        for swap, i in enumerate(pair):
            base = acc_own[level_at(i) : level_at(i) + members, :]
            put(xm, stored_at(i), members, joined(base, r_tile, at, swap))
    for floor in range(2):
        p0 = o0 = 0 if floor == 0 else 2 * HB
        x0 = 0 if floor == 0 else (HB + rows) * members
        for k in range(half):
            at = slice(p0 + k * members, p0 + (k + 1) * members)
            for swap in range(2):
                i = k + swap * half
                base = r_lev[floor, o0 + i * members : o0 + (i + 1) * members, :].astype(F32)
                put(xm, x0 + i * members, members, joined(base, r_diag.at[floor], at, swap))
    lines, own_lines = [], []
    for floor in (2, 0, 1):
        if floor == 2:
            for p0, a0 in ((pcomb_at, comb_at), (pinner_at, comb_at + 2 * HB)):
                base = acc_own[a0 : a0 + 2 * HB, :]
                own_lines.append(joined(base, r_tile, slice(p0, p0 + 2 * HB), 0))
            for i in range(rows):
                group_at, row = divmod(order.index(i), 2 * HB)
                lines.append([part[row : row + 1] for part in own_lines[group_at]])
            continue
        o0, p0 = (comb_at, pcomb_at) if floor == 0 else (0, 0)
        base = r_lev[floor, o0 : o0 + 2 * HB, :].astype(F32)
        parts = joined(base, r_diag.at[floor], slice(p0, p0 + 2 * HB), 0)
        chosen = range(HB) if floor == 0 else range(HB, 2 * HB)
        lines += [[part[i : i + 1] for part in parts] for i in chosen]
    for level in range(0, window, 2):
        for i in range(cells // LANE):
            lanes = slice(i * LANE, (i + 1) * LANE)
            both = [cp[level + s, :, lanes].astype(F32) * lines[level + s][i] for s in range(2)]
            xc[level * group : (level + 2) * group, lanes] = jnp.concatenate(both, 0).astype(BF16)

    drain(out_rim, edge * cells + 2 * pedge * LANE)


def finish(xm, xc, bm, bc, mo_hbm, co_hbm, mo, co, sem):
    rows, members, cells = mo.shape
    group = co.shape[1]
    step = rows // 2
    copies = []
    for part in range(2):
        levels = pl.ds(part * step, step)
        at = slice(part * step * members, (part + 1) * step * members)
        value = jnp.dot(bm[at, :], xm[...], preferred_element_type=F32)
        mo[levels] = value.reshape(step, members, cells)
        copies.append(pltpu.make_async_copy(mo.at[levels], mo_hbm.at[levels], sem.at[part]))
        copies[-1].start()
    left = jnp.concatenate([bc[0], bc[1]], axis=1)[:, 0 : xc.shape[0]]
    value = jnp.dot(left, xc[...], preferred_element_type=F32)
    co[...] = value.reshape(rows, group, cells)
    copies.append(pltpu.make_async_copy(co, co_hbm, sem.at[2]))
    copies[-1].start()
    for copy in copies:
        copy.wait()


def solution(mesh):
    tiles, levs = mesh.shape["tile"], mesh.shape["lev"]

    def step(members_pert, coarse_pert, member_ctrl, coarse_ctrl, vert_loc, stencil, interp_w):
        rows, members, cells = member_ctrl.shape
        group = coarse_ctrl.shape[1]
        fine = members_pert.shape[2]
        levels, span, lines = rows + 2 * HB, cells + LANE, rows * (members + 1)
        edge = HB * members + 2 * HB
        pedge = HB * members // 2 + 2 * HB
        packed = rows * members // 2 + rows
        hbm = pl.BlockSpec(memory_space=pl.ANY)
        kinds = members + 2 * group
        vmem = pl.BlockSpec(memory_space=pltpu.VMEM)
        results = pl.pallas_call(
            functools.partial(kernel, tiles, levs),
            out_shape=(
                pltpu.VMEM((levels * members, cells), BF16),
                pltpu.VMEM((levels * group, cells), BF16),
                pltpu.VMEM((rows * members, levels * members), BF16),
                pltpu.VMEM((cells // LANE, rows * group, LANE), BF16),
            ),
            in_specs=[hbm] * 7,
            out_specs=(vmem,) * 4,
            scratch_shapes=[
                pltpu.VMEM((levels, members, cells), BF16),
                pltpu.VMEM((levels, group, cells), BF16),
                pltpu.VMEM((levels, group, cells), BF16),
                pltpu.VMEM((rows, members, fine), BF16),
                pltpu.VMEM(vert_loc.shape, F32),
                pltpu.VMEM(stencil.shape, jnp.int32),
                pltpu.VMEM(interp_w.shape, BF16),
                pltpu.VMEM((fine // LANE, span, LANE), BF16),
                pltpu.VMEM((2 * cells // LANE, lines, LANE), BF16),
                pltpu.VMEM((cells // LANE, rows * group, LANE), BF16),
                pltpu.VMEM((levels, members, LANE), BF16),
                pltpu.VMEM((levels, group, LANE), BF16),
                pltpu.VMEM((rows, group, LANE), BF16),
                pltpu.VMEM((2, rows // 2, kinds, LANE), BF16),
                pltpu.VMEM((2, rows // 2, kinds, LANE), BF16),
                pltpu.VMEM((2, 2, HB // 2, members + group, LANE), BF16),
                pltpu.VMEM((cells // LANE, lines, LANE), BF16),
                pltpu.VMEM((1, lines, LANE), BF16),
                pltpu.VMEM((fine // LANE, lines, LANE), BF16),
                pltpu.VMEM((fine // LANE, rows, LANE), F32),
                pltpu.VMEM((lines, LANE), F32),
                pltpu.VMEM((edge + HB * members, cells), BF16),
                pltpu.VMEM((2, packed, LANE), BF16),
                pltpu.VMEM((lines, cells), F32),
                pltpu.VMEM((2, packed, LANE), BF16),
                pltpu.VMEM((2, edge, cells), BF16),
                pltpu.VMEM((2, 2, pedge, LANE), BF16),
                pltpu.SemaphoreType.DMA((7,)),
                pltpu.SemaphoreType.DMA((3,)),
                pltpu.SemaphoreType.DMA((5,)),
                pltpu.SemaphoreType.DMA((3,)),
                pltpu.SemaphoreType.REGULAR((2,)),
            ],
            compiler_params=pltpu.CompilerParams(
                collective_id=0, has_side_effects=True, vmem_limit_bytes=56 * 1024 * 1024
            ),
        )(members_pert, coarse_pert, member_ctrl, coarse_ctrl, vert_loc, stencil, interp_w)
        return pl.pallas_call(
            finish,
            out_shape=(
                jax.ShapeDtypeStruct((rows, members, cells), F32),
                jax.ShapeDtypeStruct((rows, group, cells), F32),
            ),
            in_specs=[vmem] * 4,
            out_specs=(hbm, hbm),
            scratch_shapes=[
                pltpu.VMEM((rows, members, cells), F32),
                pltpu.VMEM((rows, group, cells), F32),
                pltpu.SemaphoreType.DMA((3,)),
            ],
            compiler_params=pltpu.CompilerParams(vmem_limit_bytes=4 * 1024 * 1024),
        )(*results)

    in_specs = (
        P("lev", None, "tile"),
        P("lev", None, "tile"),
        P("lev", None, "tile"),
        P("lev", None, "tile"),
        P(),
        P(None, "tile"),
        P(None, "tile"),
    )
    out_specs = (P("lev", None, "tile"), P("lev", None, "tile"))
    return jax.shard_map(step, mesh=mesh, in_specs=in_specs, out_specs=out_specs, check_vma=False)
```

```python
import functools

import jax
import jax.numpy as jnp
from jax import lax
from jax.experimental import pallas as pl
from jax.experimental.pallas import tpu as pltpu
from jax.sharding import PartitionSpec as P

HB = 4
CW = 64
LANE = 128
WIDE = 2
MESH = pl.DeviceIdType.MESH
F32 = jnp.float32
BF16 = jnp.bfloat16

DIRECTIONS = ((0, -1), (0, 1), (-1, 0), (1, 0), (-1, -1), (1, -1), (-1, 1), (1, 1))


def pairs_of(rows):
    half = HB // 2
    return [(b + k, b + k + half) for b in range(0, rows, HB) for k in range(half)]


def order_of(rows):
    return list(range(rows - HB, rows)) + list(range(HB)) + list(range(HB, rows - HB))


def fold(values):
    row = lax.broadcasted_iota(jnp.int32, (8, LANE), 0)
    for stride in (1, 2, 4):
        even = (row // stride) % 2 == 0
        values = [
            jnp.where(even, a, b) + pltpu.roll(jnp.where(even, b, a), stride, 0)
            for a, b in zip(values[0::2], values[1::2])
        ]
    return values[0]


def kernel(tiles, levs, *refs):
    rows, members, cells = refs[2].shape
    group = refs[3].shape[1]
    outer, inner = 2 * HB * members + rows, (rows - 2 * HB) * members
    heights = (outer, inner, outer, inner, outer + inner, outer, rows)
    scopes = [pltpu.ACC(mxu)((height, cells), F32) for height in heights for mxu in range(2)]
    pl.run_scoped(lambda *sums: body(tiles, levs, sums, *refs), *scopes)


def body(
    tiles, levs, sums, pert_hbm, cp_hbm, mc_hbm, cc_hbm, vert_hbm, st_hbm, w_hbm, xm, xc, bm, bc,
    mc, cc, cp, pert, vert, st, w, matrix, am, ac, rim_m, rim_c, rim_p, pk, rt, rd,
    fld, fld_rim, adj, line, acc_rim, out_own, out_rim, acc_own, r_tile, r_lev, r_diag,
    load_sem, send, recv1, recv2, ready,
):
    rows, members, cells = mc_hbm.shape
    group = cc_hbm.shape[1]
    total_levels = vert_hbm.shape[0]
    fine = pert_hbm.shape[2]
    span = cells + LANE
    window = rows + 2 * HB
    edge = HB * members + 2 * HB
    last = cells - LANE
    comb_at, low_at = HB * members, HB * members + rows
    whole = rows * (members + 1)
    pcomb_at = comb_at // 2
    pedge = pcomb_at + 2 * HB
    pinner_at = rows * members // 2 + 2 * HB
    order = order_of(rows)
    pairs = pairs_of(rows)
    half = HB // 2
    kinds = members + 2 * group

    def level_at(i):
        place = order.index(i)
        return place * members + (rows if place >= HB else 0)

    assert cells == WIDE * LANE and window * members <= 2 * cells and window * group <= cells
    slots = [(sums[i : i + 2], sums[i + 2 : i + 4]) for i in (0, 4)]
    rim_sum, half_sum, few_sum = (sums[i : i + 2] for i in (8, 10, 12))
    outer, inner = 2 * HB * members + rows, (rows - 2 * HB) * members
    assert inner == rows * group
    turns = [0, 0]

    def product(into, mxu, left, right, transpose=False):
        turn = turns[mxu]
        turns[mxu] = 1 - turn
        pltpu.matmul_push_rhs(right, staging_register=turn, mxu_index=mxu, transpose=transpose)
        pltpu.matmul_acc_lhs(into[mxu], left, load_staged_rhs=turn)

    def again(into, mxu, left):
        pltpu.matmul_acc_lhs(into[mxu], left)

    t = lax.axis_index("tile")
    v = lax.axis_index("lev")
    first = v * rows
    has = {-1: v > 0, 0: None, 1: v < levs - 1}
    beside = {-1: jnp.where(t == 0, tiles - 1, t - 1), 0: t, 1: jnp.where(t == tiles - 1, 0, t + 1)}

    def when(dl, action):
        if dl == 0:
            action()
        else:
            pl.when(has[dl])(action)

    def begin(copies):
        for dl, copy in copies:
            when(dl, copy.start)

    def start_first(copies):
        for dl, copy in copies:
            pl.when(jnp.logical_and(v == 0, levs > 1))(copy.start)

    def settle(ref, sem):
        pltpu.make_async_copy(ref, ref, sem).wait()

    def filler(count):
        return pert.at[0, :, pl.ds(0, count // members)]

    def drain(ref, count):
        settle(ref, send.at[0])
        when(1, lambda: settle(filler(count), send.at[1]))
        when(-1, lambda: settle(filler(count), send.at[2]))

    own = pl.ds(0, rows)
    loads = [
        pltpu.make_async_copy(mc_hbm, mc.at[own], load_sem.at[0]),
        pltpu.make_async_copy(cc_hbm, cc.at[own], load_sem.at[0]),
        pltpu.make_async_copy(cp_hbm, cp.at[own], load_sem.at[0]),
        pltpu.make_async_copy(st_hbm, st, load_sem.at[1]),
        pltpu.make_async_copy(w_hbm, w, load_sem.at[2]),
        pltpu.make_async_copy(vert_hbm, vert, load_sem.at[3]),
        pltpu.make_async_copy(pert_hbm, pert, load_sem.at[4]),
    ]
    for load in loads[:3]:
        load.start()

    below = {-1: t > 0, 1: t == tiles - 1}

    def signal(sem, dt, dl):
        pl.semaphore_signal(sem, inc=1, device_id=(beside[dt], v + dl), device_id_type=MESH)

    barrier = pltpu.get_barrier_semaphore()
    for dt in (-1, 1):
        greets = jnp.logical_or(v <= 1, jnp.logical_not(below[dt]))
        pl.when(greets)(lambda dt=dt: signal(barrier, dt, 0))
    for dt in (-1, 0, 1):
        when(1, lambda dt=dt: signal(barrier, dt, 1))
        pl.when(v == 1)(lambda dt=dt: signal(barrier, dt, -1))
    for load in loads[3:]:
        load.start()
    pack = 16
    base_rows = lax.broadcasted_iota(jnp.int32, (pack, LANE), 0).astype(jnp.int16)

    def build(step, carry):
        lanes = pl.ds(pl.multiple_of(step * LANE, LANE), LANE)
        places, weights = [], []
        for corner in range(4):
            cell = st[corner : corner + 1, lanes] - CW
            cell = jnp.where(cell < 0, cell + span, cell)
            places.append(jnp.broadcast_to(cell, (pack, LANE)).astype(jnp.int16))
            weight = w[corner : corner + 1, lanes].astype(F32)
            weights.append(jnp.broadcast_to(weight, (pack, LANE)).astype(BF16))
        for block in range(span // pack):
            index = base_rows + jnp.int16(block * pack)
            value = jnp.zeros((pack, LANE), BF16)
            for corner in range(4):
                value = jnp.where(places[corner] == index, weights[corner], value)
            matrix[step, block * pack : (block + 1) * pack, :] = value
        return carry

    steps = fine // LANE

    def build_part(begin_at, end_at):
        if begin_at == 0:
            for load in loads[3:6]:
                load.wait()
        lax.fori_loop(begin_at, end_at, build, 0)

    def lower(shape):
        return lax.broadcasted_iota(jnp.int32, shape, len(shape) - 1) < CW

    def turned(value):
        return pltpu.roll(value, CW, 1)

    def take_loads():
        count = rows * (members + 2 * group) * cells
        settle(pert.at[pl.ds(0, count // (members * fine))], load_sem.at[0])

    def pack_rims():
        for k, (a, b) in enumerate(pairs):
            for buf, r0, rn in ((mc, 0, members), (cc, members, group), (cp, members + group, group)):
                low = lower((rn, LANE))
                near_a, near_b = (buf[i, :, 0:LANE].astype(F32) for i in (a, b))
                far_a, far_b = (buf[i, :, last:].astype(F32) for i in (a, b))
                pk[0, k, r0 : r0 + rn, :] = jnp.where(low, near_a, turned(near_b)).astype(BF16)
                pk[1, k, r0 : r0 + rn, :] = jnp.where(low, turned(far_b), far_a).astype(BF16)

    pl.when(v == 0)(lambda: build_part(0, steps // 2))

    @pl.when(v == 0)
    def _():
        take_loads()
        pack_rims()

    lower_tiles = jnp.where(t > 0, 1, 0) + jnp.where(t == tiles - 1, 1, 0)
    greeting = jnp.where(v <= 1, 2, lower_tiles)
    pl.semaphore_wait(barrier, greeting + (3 if levs > 1 else 0))
    for dt in (-1, 1):
        answers = jnp.logical_and(v > 1, below[dt])
        pl.when(answers)(lambda dt=dt: signal(ready.at[0], dt, 0))
    for dt in (-1, 0, 1):
        pl.when(v > 1)(lambda dt=dt: signal(ready.at[1], dt, -1))

    def remote(src, dst, send_at, recv_at, dt, dl):
        return dl, pltpu.make_async_remote_copy(
            src_ref=src, dst_ref=dst, send_sem=send_at, recv_sem=recv_at,
            device_id=(beside[dt], v + dl), device_id_type=MESH,
        )

    level_src = {1: rows - HB, -1: 0}
    level_dst = {1: rows, -1: rows + HB}
    entry_src = {1: len(pairs) - half, -1: 0}
    tile_row = {1: 0, -1: pcomb_at}
    lev_row = {1: 0, -1: comb_at}
    lev1, late, tile1, diag1, tile2, diag2, lev2 = [], [], [], [], [], [], []
    for dl in (-1, 1):
        floor = (1 - dl) // 2
        for buf, copies, at in ((mc, lev1, 0), (cc, lev1, 0), (cp, late, None)):
            copies.append(remote(
                buf.at[pl.ds(level_src[dl], HB)], buf.at[pl.ds(level_dst[dl], HB)],
                send.at[1 + floor], recv2.at[floor] if at is None else recv1.at[at + floor], 0, dl))
        lev2.append(remote(
            out_own.at[pl.ds(lev_row[dl], edge)], r_lev.at[floor],
            send.at[1 + floor], recv2.at[floor], 0, dl))
        for dt in (-1, 1):
            side = (1 + dt) // 2
            diag1.append(remote(
                pk.at[side, pl.ds(entry_src[dl], half), pl.ds(0, members + group)],
                rd.at[floor, side],
                send.at[1 + floor], recv1.at[2 + floor], dt, dl))
            diag2.append(remote(
                out_rim.at[side, pl.ds(tile_row[dl], pedge)], r_diag.at[floor, side],
                send.at[1 + floor], recv2.at[floor], dt, dl))
    for dt in (-1, 1):
        side = (1 + dt) // 2
        tile1.append(remote(pk.at[side], rt.at[side], send.at[0], recv1.at[4], dt, 0))
        tile2.append(remote(out_rim.at[side], r_tile.at[side], send.at[0], recv2.at[2], dt, 0))
    near = HB * (members + group) * cells
    extra = HB * group * cells

    @pl.when(v == 0)
    def _():
        for buf in (mc, cc, cp):
            buf[rows : rows + HB] = jnp.zeros((HB,) + buf.shape[1:], BF16)
        rd[0] = jnp.zeros(rd.shape[1:], BF16)
        r_lev[0] = jnp.zeros(r_lev.shape[1:], BF16)
        r_diag[0] = jnp.zeros(r_diag.shape[1:], BF16)

    @pl.when(v == levs - 1)
    def _():
        for buf in (mc, cc, cp):
            buf[rows + HB :] = jnp.zeros((HB,) + buf.shape[1:], BF16)
        rd[1] = jnp.zeros(rd.shape[1:], BF16)
        r_lev[1] = jnp.zeros(r_lev.shape[1:], BF16)
        r_diag[1] = jnp.zeros(r_diag.shape[1:], BF16)

    pl.when(v > 0)(take_loads)
    begin([x for x in lev1 if x[0] < 0])
    start_first([x for x in lev1 if x[0] > 0])
    pl.when(v > 0)(pack_rims)
    begin([x for x in diag1 if x[0] < 0])
    start_first([x for x in diag1 if x[0] > 0])
    for dt, (dl, copy) in zip((-1, 1), tile1):
        pl.when(jnp.logical_or(v <= 1, below[dt]))(copy.start)
    pl.when(v > 0)(lambda: build_part(0, steps // 2))
    asks = jnp.logical_and(v > 1, t < tiles - 1)
    pl.when(asks)(lambda: pl.semaphore_wait(ready.at[0], 2 - lower_tiles))
    for dt, (dl, copy) in zip((-1, 1), tile1):
        pl.when(jnp.logical_and(v > 1, jnp.logical_not(below[dt])))(copy.start)
    build_part(steps // 2, steps)
    factors = vert[...].astype(BF16)
    factors = jnp.concatenate(
        [factors, jnp.zeros((total_levels, cells - total_levels), BF16)], axis=1)
    factors = jnp.concatenate(
        [factors, jnp.zeros((cells - total_levels, cells), BF16)], axis=0)
    level_k = lax.broadcasted_iota(jnp.int32, (rows, cells), 1)
    level_i = lax.broadcasted_iota(jnp.int32, (rows, cells), 0)
    pick = jnp.where(level_k == first + level_i, 1.0, 0.0).astype(BF16)
    product(few_sum, 0, pick, factors)
    product(few_sum, 1, pick, factors, transpose=True)
    forward = pltpu.matmul_pop(few_sum[0]).astype(BF16)
    backward = pltpu.matmul_pop(few_sum[1]).astype(BF16)

    def spread_out(source, height, offset, mxu, base):
        shape = (total_levels, cells)
        seg = (lax.broadcasted_iota(jnp.int32, shape, 1) + base) // height
        row = lax.broadcasted_iota(jnp.int32, shape, 0)
        hit = jnp.logical_and(row == first + offset(seg), seg < window)
        chosen = jnp.where(hit, 1.0, 0.0).astype(BF16)
        chosen = jnp.concatenate([chosen, jnp.zeros((cells - total_levels, cells), BF16)], axis=0)
        product(few_sum, mxu, source, chosen)
        return pltpu.matmul_pop(few_sum[mxu])

    def blocks_of(lines, height):
        at = lax.broadcasted_iota(jnp.int32, (height, LANE), 1) % height
        mask = at == lax.broadcasted_iota(jnp.int32, (height, LANE), 0)
        return [
            [
                jnp.where(mask, line[i : i + 1, p : p + LANE], 0.0)
                for line in lines for p in range(0, cells, LANE)
            ]
            for i in range(rows)
        ]

    def natural(seg):
        halo = jnp.where(seg < rows + HB, seg - rows - HB, seg - HB)
        return jnp.where(seg < rows, seg, halo)

    def stored(seg):
        inner = jnp.where(seg < 2 * HB, seg + rows - 2 * HB, seg - 2 * HB)
        return jnp.where(jnp.logical_or(seg < HB, seg >= rows + HB), seg - HB, inner)

    lines = [spread_out(forward, members, natural, m, m * cells) for m in range(2)]
    for i, pieces in enumerate(blocks_of(lines, members)):
        for p, piece in enumerate(pieces):
            am[p, level_at(i) : level_at(i) + members, :] = piece.astype(BF16)
    for p in range(am.shape[0]):
        am[p, comb_at:low_at, :] = jnp.zeros((rows, LANE), BF16)
    lines = [spread_out(backward, members, stored, m, m * cells) for m in range(2)]
    for i, pieces in enumerate(blocks_of(lines, members)):
        for p, piece in enumerate(pieces):
            if p * LANE < bm.shape[1]:
                bm[i * members : (i + 1) * members, p * LANE : (p + 1) * LANE] = piece.astype(BF16)
    coarse_lines = [
        [spread_out(source, group, natural, m, 0)] for m, source in enumerate((forward, backward))
    ]
    for out, lines in zip((ac, bc), coarse_lines):
        blocks = blocks_of(lines, group)
        if out is ac:
            blocks = [blocks[i] for i in order]
        for i in range(0, rows, 2):
            for p in range(cells // LANE):
                both = jnp.concatenate([blocks[i][p], blocks[i + 1][p]], axis=0)
                out[p, i * group : (i + 2) * group, :] = both.astype(BF16)

    def side_by_side(ref, p0=0):
        return jnp.concatenate([ref[p0], ref[p0 + 1]], axis=1)

    def square(value):
        height, wide = value.shape
        if wide < cells:
            value = jnp.concatenate([value, jnp.zeros((height, cells - wide), BF16)], axis=1)
        if height < cells:
            value = jnp.concatenate([value, jnp.zeros((cells - height, cells), BF16)], axis=0)
        return value

    def banded(r0, r1, p0):
        return jnp.concatenate([am[p0, r0:r1, :], am[p0 + 1, r0:r1, :]], axis=1)

    def flat_of(ref, l0, l1):
        value = ref[l0:l1]
        return square(value.reshape((l1 - l0) * members, value.shape[-1]))

    def coarse_product(into, ref):
        value = ref[...].astype(F32)
        flat = value.reshape(window * group, value.shape[-1]).astype(BF16)
        product(into, 1, side_by_side(ac), square(flat))

    def put_outer(value, local, by_ref, out, wide):
        for p in range(wide // LANE):
            lanes = slice(p * LANE, (p + 1) * LANE)
            part = value[:, lanes].astype(BF16)
            out[p, 0:comb_at, :] = part[0:comb_at]
            out[p, low_at:outer, :] = part[low_at:]
            mixed = [
                local[place * group : (place + 1) * group, lanes] * by_ref[i, :, lanes].astype(F32)
                for place, i in enumerate(order)
            ]
            sums = [fold(mixed[g : g + 8]) for g in range(0, rows, 8)]
            out[p, comb_at:low_at, :] = jnp.concatenate(sums, axis=0).astype(BF16)

    def put_inner(value, out, wide):
        for p in range(wide // LANE):
            out[p, outer:, :] = value[:, p * LANE : (p + 1) * LANE].astype(BF16)

    def strip(ref, chunk, r0, r1):
        parts = [ref[chunk * WIDE + i, r0:r1, :] for i in range(WIDE)]
        return jnp.concatenate(parts, axis=1)

    def summed(value, chunk, part):
        terms = [[] for _ in range(WIDE)]
        for i in order[part * 8 : part * 8 + 8]:
            at = level_at(i) - (outer if part else 0)
            for piece in range(WIDE):
                lanes = slice(piece * LANE, (piece + 1) * LANE)
                fine_at = (chunk * WIDE + piece) * LANE
                member = pert[i, :, fine_at : fine_at + LANE].astype(F32)
                product_ = member * value[at : at + members, lanes]
                total = product_[0:8]
                for r in range(8, members, 8):
                    total = total + product_[r : r + 8]
                terms[piece].append(total)
        return [fold(term) for term in terms]

    def combined(value, piece, part):
        at = comb_at + part * 8
        return value[at : at + 8, piece * LANE : (piece + 1) * LANE]

    chunks = fine // (WIDE * LANE)

    def slot(chunk):
        return slots[(chunk // 2) % 2], chunk % 2

    def sweep(start, take, c0, c1):
        for chunk in range(c0, min(c0 + 4, c1)):
            start(chunk)
        for chunk in range(c0, c1):
            take(chunk, chunk + 4 < c1)

    def begin_inner(chunk):
        into, mxu = slot(chunk)
        product(into[1], mxu, side_by_side(fld)[outer:], strip(matrix, chunk, 0, cells))

    def take_inner(chunk, more):
        into, mxu = slot(chunk)
        value = pltpu.matmul_pop(into[1][mxu])
        if more:
            begin_inner(chunk + 4)
        for piece, total in enumerate(summed(value, chunk, 1)):
            line[chunk * WIDE + piece, 8:16, :] = total

    def begin_outer(chunk):
        into, mxu = slot(chunk)
        product(into[0], mxu, side_by_side(fld)[0:outer], strip(matrix, chunk, 0, cells))

    def take_outer(chunk, more):
        into, mxu = slot(chunk)
        value = pltpu.matmul_pop(into[0][mxu])
        if more:
            begin_outer(chunk + 4)
        for piece, total in enumerate(summed(value, chunk, 0)):
            n = chunk * WIDE + piece
            line[n, 0:8, :] = total + combined(value, piece, 0)
            line[n, 8:16, :] += combined(value, piece, 1)

    inner = jnp.logical_and(v > 0, v < levs - 1)
    pl.when(inner)(lambda: pl.semaphore_wait(ready.at[1], 3))
    for dl, copy in lev1 + diag1:
        if dl > 0:
            pl.when(inner)(copy.start)

    product(slots[0][1], 0, banded(outer, whole, 0), flat_of(mc, 0, rows))
    put_inner(pltpu.matmul_pop(slots[0][1][0]), fld, cells)
    loads[6].wait()
    sweep(begin_inner, take_inner, 0, chunks)
    when(-1, lambda: settle(filler(near), recv1.at[0]))
    when(1, lambda: settle(filler(near), recv1.at[1]))
    begin(late)
    (first_outer, first_inner), _ = slots
    product(first_outer, 0, banded(0, outer, 0), flat_of(mc, 0, rows))
    product(first_outer, 1, banded(0, outer, 2), flat_of(mc, rows, window))
    coarse_product(first_inner, cc)
    value = pltpu.matmul_pop(first_outer[0]) + pltpu.matmul_pop(first_outer[1])
    put_outer(value, pltpu.matmul_pop(first_inner[1]), cp, fld, cells)
    sweep(begin_outer, take_outer, 0, chunks)
    def unpack(from_next, from_prev):
        low = lower(from_next.shape)
        nxt, prv = from_next.astype(F32), from_prev.astype(F32)
        return jnp.where(low, nxt, prv), turned(jnp.where(low, prv, nxt))

    def keep(level, value):
        value = value.astype(BF16)
        rim_m[level] = value[0:members]
        rim_c[level] = value[members : members + group]
        if level < rows:
            rim_p[level] = value[members + group :]

    settle(rt, recv1.at[4])
    for k, (a, b) in enumerate(pairs):
        va, vb = unpack(rt[0, k], rt[1, k])
        keep(a, va)
        keep(b, vb)
    product(half_sum, 0, banded(0, outer, 0), flat_of(rim_m, 0, rows))
    again(first_inner, 0, banded(outer, whole, 0))
    when(-1, lambda: settle(rd.at[0], recv1.at[2]))
    when(1, lambda: settle(rd.at[1], recv1.at[3]))
    for floor in range(2):
        for k in range(half):
            va, vb = unpack(rd[floor, 0, k], rd[floor, 1, k])
            base = rows + floor * HB
            keep(base + k, va)
            keep(base + k + half, vb)
    product(half_sum, 1, banded(0, outer, 2), flat_of(rim_m, rows, window))
    coarse_product(first_inner, rim_c)
    value = pltpu.matmul_pop(half_sum[0]) + pltpu.matmul_pop(half_sum[1])
    put_inner(pltpu.matmul_pop(first_inner[0]), fld_rim, LANE)
    put_outer(value, pltpu.matmul_pop(first_inner[1]), rim_p, fld_rim, LANE)
    rim_fields = jnp.concatenate([fld_rim[0], jnp.zeros((whole, cells - LANE), BF16)], axis=1)
    def rim_of(chunk):
        return square(strip(matrix, chunk, cells, span))

    def begin_rim(chunk):
        into, mxu = slot(chunk)
        product(into[0], mxu, rim_fields[0:outer], rim_of(chunk))
        again(into[1], mxu, rim_fields[outer:])

    def rim_and_first(chunk):
        value = [strip(matrix, chunk, cells, span), strip(matrix, chunk, 0, LANE)]
        return jnp.concatenate(value, axis=0)

    def second_half(chunk):
        return square(strip(matrix, chunk, LANE, cells))

    def take_rim(chunk, more):
        into, mxu = slot(chunk)
        values = [pltpu.matmul_pop(into[part][mxu]) for part in range(2)]
        if more:
            begin_rim(chunk + 4)
        totals = [[] for _ in range(WIDE)]
        for part in range(2):
            for piece, total in enumerate(summed(values[part], chunk, part)):
                n = chunk * WIDE + piece
                total = total + combined(values[0], piece, part)
                total = total + line[n, part * 8 : part * 8 + 8, :]
                totals[piece].append(total)
                for r, i in enumerate(order[part * 8 : part * 8 + 8]):
                    by = jnp.broadcast_to(total[r : r + 1], (members, LANE)).astype(BF16)
                    at = level_at(i)
                    lanes = slice(n * LANE, (n + 1) * LANE)
                    adj[n, at : at + members, :] = pert[i, :, lanes] * by
        for piece in range(WIDE):
            both = jnp.concatenate(totals[piece], axis=0)
            adj[chunk * WIDE + piece, comb_at:low_at, :] = both.astype(BF16)
        product(rim_sum, mxu, strip(adj, chunk, 0, whole), rim_and_first(chunk), transpose=True)
        product(half_sum, mxu, strip(adj, chunk, 0, outer), second_half(chunk), transpose=True)

    sweep(begin_rim, take_rim, 0, chunks)
    back = pltpu.matmul_pop(rim_sum[0]) + pltpu.matmul_pop(rim_sum[1])
    acc_rim[...] = back[:, 0:LANE]
    acc_own[:, 0:LANE] = back[:, LANE:]
    back = pltpu.matmul_pop(half_sum[0]) + pltpu.matmul_pop(half_sum[1])
    acc_own[0:outer, LANE:] = back[:, 0:LANE]
    out_own[0:edge, :] = acc_own[0:edge, :].astype(BF16)
    out_own[edge:, :] = acc_own[low_at:outer, :].astype(BF16)
    def packed_at(k):
        place = order.index(pairs[k][0])
        entry = place // HB * half + place % HB
        return entry * members + (2 * HB if place >= HB else 0)

    low = lower((members, LANE))
    for k, (a, b) in enumerate(pairs):
        value_a = acc_rim[level_at(a) : level_at(a) + members, :]
        value_b = turned(acc_rim[level_at(b) : level_at(b) + members, :])
        at = slice(packed_at(k), packed_at(k) + members)
        out_rim[1, at, :] = jnp.where(low, value_a, value_b).astype(BF16)
        out_rim[0, at, :] = jnp.where(low, value_b, value_a).astype(BF16)
    for side in range(2):
        both = acc_rim[comb_at:low_at, :].astype(BF16)
        out_rim[side, pcomb_at : pcomb_at + 2 * HB, :] = both[0 : 2 * HB]
        out_rim[side, pinner_at:, :] = both[2 * HB :]

    drain(pk, near + extra + 2 * half * (members + group) * LANE)
    begin([x for x in diag2 + lev2 if x[0] < 0] + tile2)
    for chunk in range(chunks):
        part = strip(adj, chunk, outer, whole)
        product(first_inner, chunk % 2, part, second_half(chunk), transpose=True)
    back = pltpu.matmul_pop(first_inner[0]) + pltpu.matmul_pop(first_inner[1])
    acc_own[outer:, LANE:] = back[:, 0:LANE]
    begin([x for x in diag2 + lev2 if x[0] > 0])
    settle(r_tile, recv2.at[2])
    far = extra + edge * cells + 2 * pedge * LANE
    when(-1, lambda: settle(filler(far), recv2.at[0]))
    when(1, lambda: settle(filler(far), recv2.at[1]))
    def zero_but(value, keep_low):
        low = lower(value.shape)
        return jnp.where(low, value, 0.0) if keep_low else jnp.where(low, 0.0, value)

    def joined(base, messages, at, swap):
        from_prev, from_next = messages[1, at, :].astype(F32), messages[0, at, :].astype(F32)
        if swap:
            from_prev, from_next = turned(from_prev), turned(from_next)
        parts = [base[:, i * LANE : (i + 1) * LANE] for i in range(cells // LANE)]
        parts[0] = parts[0] + zero_but(from_prev, True)
        parts[-1] = parts[-1] + zero_but(from_next, False)
        return parts

    def put(ref, r0, rn, parts):
        for i, part in enumerate(parts):
            ref[r0 : r0 + rn, i * LANE : (i + 1) * LANE] = part.astype(BF16)

    def stored_at(i):
        return (HB + order.index(i)) * members

    for k, pair in enumerate(pairs):
        at = slice(packed_at(k), packed_at(k) + members)
        for swap, i in enumerate(pair):
            base = acc_own[level_at(i) : level_at(i) + members, :]
            put(xm, stored_at(i), members, joined(base, r_tile, at, swap))
    for floor in range(2):
        p0 = o0 = 0 if floor == 0 else 2 * HB
        x0 = 0 if floor == 0 else (HB + rows) * members
        for k in range(half):
            at = slice(p0 + k * members, p0 + (k + 1) * members)
            for swap in range(2):
                i = k + swap * half
                base = r_lev[floor, o0 + i * members : o0 + (i + 1) * members, :].astype(F32)
                put(xm, x0 + i * members, members, joined(base, r_diag.at[floor], at, swap))
    lines, own_lines = [], []
    for floor in (2, 0, 1):
        if floor == 2:
            for p0, a0 in ((pcomb_at, comb_at), (pinner_at, comb_at + 2 * HB)):
                base = acc_own[a0 : a0 + 2 * HB, :]
                own_lines.append(joined(base, r_tile, slice(p0, p0 + 2 * HB), 0))
            for i in range(rows):
                group_at, row = divmod(order.index(i), 2 * HB)
                lines.append([part[row : row + 1] for part in own_lines[group_at]])
            continue
        o0, p0 = (comb_at, pcomb_at) if floor == 0 else (0, 0)
        base = r_lev[floor, o0 : o0 + 2 * HB, :].astype(F32)
        parts = joined(base, r_diag.at[floor], slice(p0, p0 + 2 * HB), 0)
        chosen = range(HB) if floor == 0 else range(HB, 2 * HB)
        lines += [[part[i : i + 1] for part in parts] for i in chosen]
    for level in range(0, window, 2):
        for i in range(cells // LANE):
            lanes = slice(i * LANE, (i + 1) * LANE)
            both = [cp[level + s, :, lanes].astype(F32) * lines[level + s][i] for s in range(2)]
            xc[level * group : (level + 2) * group, lanes] = jnp.concatenate(both, 0).astype(BF16)

    drain(out_rim, edge * cells + 2 * pedge * LANE)


def finish(xm, xc, bm, bc, mo_hbm, co_hbm, mo, co, sem):
    rows, members, cells = mo.shape
    group = co.shape[1]
    copies, pieces = [], 4
    step = rows // pieces
    left = jnp.concatenate([bc[0], bc[1]], axis=1)[:, 0 : xc.shape[0]]
    value = jnp.dot(left, xc[...], preferred_element_type=F32)
    co[...] = value.reshape(rows, group, cells)
    copies.append(pltpu.make_async_copy(co, co_hbm, sem.at[pieces]))
    copies[-1].start()
    for part in range(pieces):
        levels = pl.ds(part * step, step)
        at = slice(part * step * members, (part + 1) * step * members)
        value = jnp.dot(bm[at, :], xm[...], preferred_element_type=F32)
        mo[levels] = value.reshape(step, members, cells)
        copies.append(pltpu.make_async_copy(mo.at[levels], mo_hbm.at[levels], sem.at[part]))
        copies[-1].start()
    for copy in copies:
        copy.wait()


def solution(mesh):
    tiles, levs = mesh.shape["tile"], mesh.shape["lev"]

    def step(members_pert, coarse_pert, member_ctrl, coarse_ctrl, vert_loc, stencil, interp_w):
        rows, members, cells = member_ctrl.shape
        group = coarse_ctrl.shape[1]
        fine = members_pert.shape[2]
        levels, span, lines = rows + 2 * HB, cells + LANE, rows * (members + 1)
        edge = HB * members + 2 * HB
        pedge = HB * members // 2 + 2 * HB
        packed = rows * members // 2 + rows
        hbm = pl.BlockSpec(memory_space=pl.ANY)
        kinds = members + 2 * group
        vmem = pl.BlockSpec(memory_space=pltpu.VMEM)
        results = pl.pallas_call(
            functools.partial(kernel, tiles, levs),
            out_shape=(
                pltpu.VMEM((levels * members, cells), BF16),
                pltpu.VMEM((levels * group, cells), BF16),
                pltpu.VMEM((rows * members, levels * members), BF16),
                pltpu.VMEM((cells // LANE, rows * group, LANE), BF16),
            ),
            in_specs=[hbm] * 7,
            out_specs=(vmem,) * 4,
            scratch_shapes=[
                pltpu.VMEM((levels, members, cells), BF16),
                pltpu.VMEM((levels, group, cells), BF16),
                pltpu.VMEM((levels, group, cells), BF16),
                pltpu.VMEM((rows, members, fine), BF16),
                pltpu.VMEM(vert_loc.shape, F32),
                pltpu.VMEM(stencil.shape, jnp.int32),
                pltpu.VMEM(interp_w.shape, BF16),
                pltpu.VMEM((fine // LANE, span, LANE), BF16),
                pltpu.VMEM((2 * cells // LANE, lines, LANE), BF16),
                pltpu.VMEM((cells // LANE, rows * group, LANE), BF16),
                pltpu.VMEM((levels, members, LANE), BF16),
                pltpu.VMEM((levels, group, LANE), BF16),
                pltpu.VMEM((rows, group, LANE), BF16),
                pltpu.VMEM((2, rows // 2, kinds, LANE), BF16),
                pltpu.VMEM((2, rows // 2, kinds, LANE), BF16),
                pltpu.VMEM((2, 2, HB // 2, members + group, LANE), BF16),
                pltpu.VMEM((cells // LANE, lines, LANE), BF16),
                pltpu.VMEM((1, lines, LANE), BF16),
                pltpu.VMEM((fine // LANE, lines, LANE), BF16),
                pltpu.VMEM((fine // LANE, rows, LANE), F32),
                pltpu.VMEM((lines, LANE), F32),
                pltpu.VMEM((edge + HB * members, cells), BF16),
                pltpu.VMEM((2, packed, LANE), BF16),
                pltpu.VMEM((lines, cells), F32),
                pltpu.VMEM((2, packed, LANE), BF16),
                pltpu.VMEM((2, edge, cells), BF16),
                pltpu.VMEM((2, 2, pedge, LANE), BF16),
                pltpu.SemaphoreType.DMA((5,)),
                pltpu.SemaphoreType.DMA((3,)),
                pltpu.SemaphoreType.DMA((5,)),
                pltpu.SemaphoreType.DMA((3,)),
                pltpu.SemaphoreType.REGULAR((2,)),
            ],
            compiler_params=pltpu.CompilerParams(
                collective_id=0, has_side_effects=True, vmem_limit_bytes=56 * 1024 * 1024
            ),
        )(members_pert, coarse_pert, member_ctrl, coarse_ctrl, vert_loc, stencil, interp_w)
        return pl.pallas_call(
            finish,
            out_shape=(
                jax.ShapeDtypeStruct((rows, members, cells), F32),
                jax.ShapeDtypeStruct((rows, group, cells), F32),
            ),
            in_specs=[vmem] * 4,
            out_specs=(hbm, hbm),
            scratch_shapes=[
                pltpu.VMEM((rows, members, cells), F32),
                pltpu.VMEM((rows, group, cells), F32),
                pltpu.SemaphoreType.DMA((5,)),
            ],
            compiler_params=pltpu.CompilerParams(vmem_limit_bytes=4 * 1024 * 1024),
        )(*results)

    in_specs = (
        P("lev", None, "tile"),
        P("lev", None, "tile"),
        P("lev", None, "tile"),
        P("lev", None, "tile"),
        P(),
        P(None, "tile"),
        P(None, "tile"),
    )
    out_specs = (P("lev", None, "tile"), P("lev", None, "tile"))
    return jax.shard_map(step, mesh=mesh, in_specs=in_specs, out_specs=out_specs, check_vma=False)
```

```python
import functools

import jax
import jax.numpy as jnp
from jax import lax
from jax.experimental import pallas as pl
from jax.experimental.pallas import tpu as pltpu
from jax.sharding import PartitionSpec as P

HB = 4
CW = 64
LANE = 128
WIDE = 2
MESH = pl.DeviceIdType.MESH
F32 = jnp.float32
BF16 = jnp.bfloat16

DIRECTIONS = ((0, -1), (0, 1), (-1, 0), (1, 0), (-1, -1), (1, -1), (-1, 1), (1, 1))


def pairs_of(rows):
    half = HB // 2
    return [(b + k, b + k + half) for b in range(0, rows, HB) for k in range(half)]


def order_of(rows):
    return list(range(rows - HB, rows)) + list(range(HB)) + list(range(HB, rows - HB))


def fold(values):
    row = lax.broadcasted_iota(jnp.int32, (8, LANE), 0)
    for stride in (1, 2, 4):
        even = (row // stride) % 2 == 0
        values = [
            jnp.where(even, a, b) + pltpu.roll(jnp.where(even, b, a), stride, 0)
            for a, b in zip(values[0::2], values[1::2])
        ]
    return values[0]


def kernel(tiles, levs, *refs):
    rows, members, cells = refs[2].shape
    group = refs[3].shape[1]
    outer, inner = 2 * HB * members + rows, (rows - 2 * HB) * members
    heights = (outer, inner, outer, inner, outer + inner, outer, rows)
    scopes = [pltpu.ACC(mxu)((height, cells), F32) for height in heights for mxu in range(2)]
    pl.run_scoped(lambda *sums: body(tiles, levs, sums, *refs), *scopes)


def body(
    tiles, levs, sums, pert_hbm, cp_hbm, mc_hbm, cc_hbm, vert_hbm, st_hbm, w_hbm, xm, xc, bm, bc,
    mc, cc, cp, pert, vert, st, w, matrix, am, ac, rim_m, rim_c, rim_p, pk, rt, rd,
    fld, fld_rim, adj, line, acc_rim, out_own, out_rim, acc_own, r_tile, r_lev, r_diag,
    load_sem, send, recv1, recv2, ready,
):
    rows, members, cells = mc_hbm.shape
    group = cc_hbm.shape[1]
    total_levels = vert_hbm.shape[0]
    fine = pert_hbm.shape[2]
    span = cells + LANE
    window = rows + 2 * HB
    edge = HB * members + 2 * HB
    last = cells - LANE
    comb_at, low_at = HB * members, HB * members + rows
    whole = rows * (members + 1)
    pcomb_at = comb_at // 2
    pedge = pcomb_at + 2 * HB
    pinner_at = rows * members // 2 + 2 * HB
    order = order_of(rows)
    pairs = pairs_of(rows)
    half = HB // 2
    kinds = members + 2 * group

    def level_at(i):
        place = order.index(i)
        return place * members + (rows if place >= HB else 0)

    assert cells == WIDE * LANE and window * members <= 2 * cells and window * group <= cells
    slots = [(sums[i : i + 2], sums[i + 2 : i + 4]) for i in (0, 4)]
    rim_sum, half_sum, few_sum = (sums[i : i + 2] for i in (8, 10, 12))
    outer, inner = 2 * HB * members + rows, (rows - 2 * HB) * members
    assert inner == rows * group
    turns = [0, 0]

    def product(into, mxu, left, right, transpose=False):
        turn = turns[mxu]
        turns[mxu] = 1 - turn
        pltpu.matmul_push_rhs(right, staging_register=turn, mxu_index=mxu, transpose=transpose)
        pltpu.matmul_acc_lhs(into[mxu], left, load_staged_rhs=turn)

    def again(into, mxu, left):
        pltpu.matmul_acc_lhs(into[mxu], left)

    t = lax.axis_index("tile")
    v = lax.axis_index("lev")
    first = v * rows
    has = {-1: v > 0, 0: None, 1: v < levs - 1}
    beside = {-1: jnp.where(t == 0, tiles - 1, t - 1), 0: t, 1: jnp.where(t == tiles - 1, 0, t + 1)}

    def when(dl, action):
        if dl == 0:
            action()
        else:
            pl.when(has[dl])(action)

    def begin(copies):
        for dl, copy in copies:
            when(dl, copy.start)

    def start_first(copies):
        for dl, copy in copies:
            pl.when(jnp.logical_and(v == 0, levs > 1))(copy.start)

    def settle(ref, sem):
        pltpu.make_async_copy(ref, ref, sem).wait()

    def filler(count):
        return pert.at[0, :, pl.ds(0, count // members)]

    def drain(ref, count):
        settle(ref, send.at[0])
        when(1, lambda: settle(filler(count), send.at[1]))
        when(-1, lambda: settle(filler(count), send.at[2]))

    own = pl.ds(0, rows)
    loads = [
        pltpu.make_async_copy(mc_hbm, mc.at[own], load_sem.at[0]),
        pltpu.make_async_copy(cc_hbm, cc.at[own], load_sem.at[0]),
        pltpu.make_async_copy(cp_hbm, cp.at[own], load_sem.at[0]),
        pltpu.make_async_copy(st_hbm, st, load_sem.at[1]),
        pltpu.make_async_copy(w_hbm, w, load_sem.at[2]),
        pltpu.make_async_copy(vert_hbm, vert, load_sem.at[3]),
        pltpu.make_async_copy(pert_hbm, pert, load_sem.at[4]),
    ]
    for load in loads[:3]:
        load.start()

    below = {-1: t > 0, 1: t == tiles - 1}

    def signal(sem, dt, dl):
        pl.semaphore_signal(sem, inc=1, device_id=(beside[dt], v + dl), device_id_type=MESH)

    barrier = pltpu.get_barrier_semaphore()
    for dt in (-1, 1):
        greets = jnp.logical_or(v <= 1, jnp.logical_not(below[dt]))
        pl.when(greets)(lambda dt=dt: signal(barrier, dt, 0))
    for dt in (-1, 0, 1):
        when(1, lambda dt=dt: signal(barrier, dt, 1))
        pl.when(v == 1)(lambda dt=dt: signal(barrier, dt, -1))
    for load in loads[3:]:
        load.start()
    pack = 16
    base_rows = lax.broadcasted_iota(jnp.int32, (pack, LANE), 0).astype(jnp.int16)

    def build(step, carry):
        lanes = pl.ds(pl.multiple_of(step * LANE, LANE), LANE)
        places, weights = [], []
        for corner in range(4):
            cell = st[corner : corner + 1, lanes] - CW
            cell = jnp.where(cell < 0, cell + span, cell)
            places.append(jnp.broadcast_to(cell, (pack, LANE)).astype(jnp.int16))
            weight = w[corner : corner + 1, lanes].astype(F32)
            weights.append(jnp.broadcast_to(weight, (pack, LANE)).astype(BF16))
        for block in range(span // pack):
            index = base_rows + jnp.int16(block * pack)
            value = jnp.zeros((pack, LANE), BF16)
            for corner in range(4):
                value = jnp.where(places[corner] == index, weights[corner], value)
            matrix[step, block * pack : (block + 1) * pack, :] = value
        return carry

    steps = fine // LANE

    def build_part(begin_at, end_at):
        if begin_at == 0:
            for load in loads[3:6]:
                load.wait()
        lax.fori_loop(begin_at, end_at, build, 0)

    def lower(shape):
        return lax.broadcasted_iota(jnp.int32, shape, len(shape) - 1) < CW

    def turned(value):
        return pltpu.roll(value, CW, 1)

    def take_loads():
        count = rows * (members + 2 * group) * cells
        settle(pert.at[pl.ds(0, count // (members * fine))], load_sem.at[0])

    def pack_rims():
        for k, (a, b) in enumerate(pairs):
            for buf, r0, rn in ((mc, 0, members), (cc, members, group), (cp, members + group, group)):
                low = lower((rn, LANE))
                near_a, near_b = (buf[i, :, 0:LANE].astype(F32) for i in (a, b))
                far_a, far_b = (buf[i, :, last:].astype(F32) for i in (a, b))
                pk[0, k, r0 : r0 + rn, :] = jnp.where(low, near_a, turned(near_b)).astype(BF16)
                pk[1, k, r0 : r0 + rn, :] = jnp.where(low, turned(far_b), far_a).astype(BF16)

    pl.when(v == 0)(lambda: build_part(0, steps // 2))

    @pl.when(v == 0)
    def _():
        take_loads()
        pack_rims()

    lower_tiles = jnp.where(t > 0, 1, 0) + jnp.where(t == tiles - 1, 1, 0)
    greeting = jnp.where(v <= 1, 2, lower_tiles)
    pl.semaphore_wait(barrier, greeting + (3 if levs > 1 else 0))
    for dt in (-1, 1):
        answers = jnp.logical_and(v > 1, below[dt])
        pl.when(answers)(lambda dt=dt: signal(ready.at[0], dt, 0))
    for dt in (-1, 0, 1):
        pl.when(v > 1)(lambda dt=dt: signal(ready.at[1], dt, -1))

    def remote(src, dst, send_at, recv_at, dt, dl):
        return dl, pltpu.make_async_remote_copy(
            src_ref=src, dst_ref=dst, send_sem=send_at, recv_sem=recv_at,
            device_id=(beside[dt], v + dl), device_id_type=MESH,
        )

    level_src = {1: rows - HB, -1: 0}
    level_dst = {1: rows, -1: rows + HB}
    entry_src = {1: len(pairs) - half, -1: 0}
    tile_row = {1: 0, -1: pcomb_at}
    lev_row = {1: 0, -1: comb_at}
    lev1, late, tile1, diag1, tile2, diag2, lev2 = [], [], [], [], [], [], []
    for dl in (-1, 1):
        floor = (1 - dl) // 2
        for buf, copies, at in ((mc, lev1, 0), (cc, lev1, 0), (cp, late, None)):
            copies.append(remote(
                buf.at[pl.ds(level_src[dl], HB)], buf.at[pl.ds(level_dst[dl], HB)],
                send.at[1 + floor], recv2.at[floor] if at is None else recv1.at[at + floor], 0, dl))
        lev2.append(remote(
            out_own.at[pl.ds(lev_row[dl], edge)], r_lev.at[floor],
            send.at[1 + floor], recv2.at[floor], 0, dl))
        for dt in (-1, 1):
            side = (1 + dt) // 2
            diag1.append(remote(
                pk.at[side, pl.ds(entry_src[dl], half), pl.ds(0, members + group)],
                rd.at[floor, side],
                send.at[1 + floor], recv1.at[2 + floor], dt, dl))
            diag2.append(remote(
                out_rim.at[side, pl.ds(tile_row[dl], pedge)], r_diag.at[floor, side],
                send.at[1 + floor], recv2.at[floor], dt, dl))
    for dt in (-1, 1):
        side = (1 + dt) // 2
        tile1.append(remote(pk.at[side], rt.at[side], send.at[0], recv1.at[4], dt, 0))
        tile2.append(remote(out_rim.at[side], r_tile.at[side], send.at[0], recv2.at[2], dt, 0))
    near = HB * (members + group) * cells
    extra = HB * group * cells

    @pl.when(v == 0)
    def _():
        for buf in (mc, cc, cp):
            buf[rows : rows + HB] = jnp.zeros((HB,) + buf.shape[1:], BF16)
        rd[0] = jnp.zeros(rd.shape[1:], BF16)
        r_lev[0] = jnp.zeros(r_lev.shape[1:], BF16)
        r_diag[0] = jnp.zeros(r_diag.shape[1:], BF16)

    @pl.when(v == levs - 1)
    def _():
        for buf in (mc, cc, cp):
            buf[rows + HB :] = jnp.zeros((HB,) + buf.shape[1:], BF16)
        rd[1] = jnp.zeros(rd.shape[1:], BF16)
        r_lev[1] = jnp.zeros(r_lev.shape[1:], BF16)
        r_diag[1] = jnp.zeros(r_diag.shape[1:], BF16)

    pl.when(v > 0)(take_loads)
    begin([x for x in lev1 if x[0] < 0])
    start_first([x for x in lev1 if x[0] > 0])
    pl.when(v > 0)(pack_rims)
    begin([x for x in diag1 if x[0] < 0])
    start_first([x for x in diag1 if x[0] > 0])
    for dt, (dl, copy) in zip((-1, 1), tile1):
        pl.when(jnp.logical_or(v <= 1, below[dt]))(copy.start)
    pl.when(v > 0)(lambda: build_part(0, steps // 2))
    asks = jnp.logical_and(v > 1, t < tiles - 1)
    pl.when(asks)(lambda: pl.semaphore_wait(ready.at[0], 2 - lower_tiles))
    for dt, (dl, copy) in zip((-1, 1), tile1):
        pl.when(jnp.logical_and(v > 1, jnp.logical_not(below[dt])))(copy.start)
    build_part(steps // 2, steps)
    factors = vert[...].astype(BF16)
    factors = jnp.concatenate(
        [factors, jnp.zeros((total_levels, cells - total_levels), BF16)], axis=1)
    factors = jnp.concatenate(
        [factors, jnp.zeros((cells - total_levels, cells), BF16)], axis=0)
    level_k = lax.broadcasted_iota(jnp.int32, (rows, cells), 1)
    level_i = lax.broadcasted_iota(jnp.int32, (rows, cells), 0)
    pick = jnp.where(level_k == first + level_i, 1.0, 0.0).astype(BF16)
    product(few_sum, 0, pick, factors)
    product(few_sum, 1, pick, factors, transpose=True)
    forward = pltpu.matmul_pop(few_sum[0]).astype(BF16)
    backward = pltpu.matmul_pop(few_sum[1]).astype(BF16)

    def spread_out(source, height, offset, mxu, base):
        shape = (total_levels, cells)
        seg = (lax.broadcasted_iota(jnp.int32, shape, 1) + base) // height
        row = lax.broadcasted_iota(jnp.int32, shape, 0)
        hit = jnp.logical_and(row == first + offset(seg), seg < window)
        chosen = jnp.where(hit, 1.0, 0.0).astype(BF16)
        chosen = jnp.concatenate([chosen, jnp.zeros((cells - total_levels, cells), BF16)], axis=0)
        product(few_sum, mxu, source, chosen)
        return pltpu.matmul_pop(few_sum[mxu])

    def blocks_of(lines, height):
        at = lax.broadcasted_iota(jnp.int32, (height, LANE), 1) % height
        mask = at == lax.broadcasted_iota(jnp.int32, (height, LANE), 0)
        return [
            [
                jnp.where(mask, line[i : i + 1, p : p + LANE], 0.0)
                for line in lines for p in range(0, cells, LANE)
            ]
            for i in range(rows)
        ]

    def natural(seg):
        halo = jnp.where(seg < rows + HB, seg - rows - HB, seg - HB)
        return jnp.where(seg < rows, seg, halo)

    def stored(seg):
        inner = jnp.where(seg < 2 * HB, seg + rows - 2 * HB, seg - 2 * HB)
        return jnp.where(jnp.logical_or(seg < HB, seg >= rows + HB), seg - HB, inner)

    lines = [spread_out(forward, members, natural, m, m * cells) for m in range(2)]
    for i, pieces in enumerate(blocks_of(lines, members)):
        for p, piece in enumerate(pieces):
            am[p, level_at(i) : level_at(i) + members, :] = piece.astype(BF16)
    for p in range(am.shape[0]):
        am[p, comb_at:low_at, :] = jnp.zeros((rows, LANE), BF16)
    lines = [spread_out(backward, members, stored, m, m * cells) for m in range(2)]
    for i, pieces in enumerate(blocks_of(lines, members)):
        for p, piece in enumerate(pieces):
            if p * LANE < bm.shape[1]:
                bm[i * members : (i + 1) * members, p * LANE : (p + 1) * LANE] = piece.astype(BF16)
    coarse_lines = [
        [spread_out(source, group, natural, m, 0)] for m, source in enumerate((forward, backward))
    ]
    for out, lines in zip((ac, bc), coarse_lines):
        blocks = blocks_of(lines, group)
        if out is ac:
            blocks = [blocks[i] for i in order]
        for i in range(0, rows, 2):
            for p in range(cells // LANE):
                both = jnp.concatenate([blocks[i][p], blocks[i + 1][p]], axis=0)
                out[p, i * group : (i + 2) * group, :] = both.astype(BF16)

    def side_by_side(ref, p0=0):
        return jnp.concatenate([ref[p0], ref[p0 + 1]], axis=1)

    def square(value):
        height, wide = value.shape
        if wide < cells:
            value = jnp.concatenate([value, jnp.zeros((height, cells - wide), BF16)], axis=1)
        if height < cells:
            value = jnp.concatenate([value, jnp.zeros((cells - height, cells), BF16)], axis=0)
        return value

    def banded(r0, r1, p0):
        return jnp.concatenate([am[p0, r0:r1, :], am[p0 + 1, r0:r1, :]], axis=1)

    def flat_of(ref, l0, l1):
        value = ref[l0:l1]
        return square(value.reshape((l1 - l0) * members, value.shape[-1]))

    def coarse_product(into, ref):
        value = ref[...].astype(F32)
        flat = value.reshape(window * group, value.shape[-1]).astype(BF16)
        product(into, 1, side_by_side(ac), square(flat))

    def put_outer(value, local, by_ref, out, wide):
        for p in range(wide // LANE):
            lanes = slice(p * LANE, (p + 1) * LANE)
            part = value[:, lanes].astype(BF16)
            out[p, 0:comb_at, :] = part[0:comb_at]
            out[p, low_at:outer, :] = part[low_at:]
            mixed = [
                local[place * group : (place + 1) * group, lanes] * by_ref[i, :, lanes].astype(F32)
                for place, i in enumerate(order)
            ]
            sums = [fold(mixed[g : g + 8]) for g in range(0, rows, 8)]
            out[p, comb_at:low_at, :] = jnp.concatenate(sums, axis=0).astype(BF16)

    def put_inner(value, out, wide):
        for p in range(wide // LANE):
            out[p, outer:, :] = value[:, p * LANE : (p + 1) * LANE].astype(BF16)

    def strip(ref, chunk, r0, r1):
        parts = [ref[chunk * WIDE + i, r0:r1, :] for i in range(WIDE)]
        return jnp.concatenate(parts, axis=1)

    def summed(value, chunk, part):
        terms = [[] for _ in range(WIDE)]
        for i in order[part * 8 : part * 8 + 8]:
            at = level_at(i) - (outer if part else 0)
            for piece in range(WIDE):
                lanes = slice(piece * LANE, (piece + 1) * LANE)
                fine_at = (chunk * WIDE + piece) * LANE
                member = pert[i, :, fine_at : fine_at + LANE].astype(F32)
                product_ = member * value[at : at + members, lanes]
                total = product_[0:8]
                for r in range(8, members, 8):
                    total = total + product_[r : r + 8]
                terms[piece].append(total)
        return [fold(term) for term in terms]

    def combined(value, piece, part):
        at = comb_at + part * 8
        return value[at : at + 8, piece * LANE : (piece + 1) * LANE]

    chunks = fine // (WIDE * LANE)

    def slot(chunk):
        return slots[(chunk // 2) % 2], chunk % 2

    def sweep(start, take, c0, c1):
        for chunk in range(c0, min(c0 + 4, c1)):
            start(chunk)
        for chunk in range(c0, c1):
            take(chunk, chunk + 4 < c1)

    def begin_inner(chunk):
        into, mxu = slot(chunk)
        product(into[1], mxu, side_by_side(fld)[outer:], strip(matrix, chunk, 0, cells))

    def take_inner(chunk, more):
        into, mxu = slot(chunk)
        value = pltpu.matmul_pop(into[1][mxu])
        if more:
            begin_inner(chunk + 4)
        for piece, total in enumerate(summed(value, chunk, 1)):
            line[chunk * WIDE + piece, 8:16, :] = total

    def begin_outer(chunk):
        into, mxu = slot(chunk)
        product(into[0], mxu, side_by_side(fld)[0:outer], strip(matrix, chunk, 0, cells))

    def take_outer(chunk, more):
        into, mxu = slot(chunk)
        value = pltpu.matmul_pop(into[0][mxu])
        if more:
            begin_outer(chunk + 4)
        for piece, total in enumerate(summed(value, chunk, 0)):
            n = chunk * WIDE + piece
            line[n, 0:8, :] = total + combined(value, piece, 0)
            line[n, 8:16, :] += combined(value, piece, 1)

    inner = jnp.logical_and(v > 0, v < levs - 1)
    pl.when(inner)(lambda: pl.semaphore_wait(ready.at[1], 3))
    for dl, copy in lev1 + diag1:
        if dl > 0:
            pl.when(inner)(copy.start)

    product(slots[0][1], 0, banded(outer, whole, 0), flat_of(mc, 0, rows))
    put_inner(pltpu.matmul_pop(slots[0][1][0]), fld, cells)
    loads[6].wait()
    sweep(begin_inner, take_inner, 0, chunks)
    when(-1, lambda: settle(filler(near), recv1.at[0]))
    when(1, lambda: settle(filler(near), recv1.at[1]))
    (first_outer, first_inner), _ = slots
    product(first_outer, 0, banded(0, outer, 0), flat_of(mc, 0, rows))
    product(first_outer, 1, banded(0, outer, 2), flat_of(mc, rows, window))
    coarse_product(first_inner, cc)
    value = pltpu.matmul_pop(first_outer[0]) + pltpu.matmul_pop(first_outer[1])
    put_outer(value, pltpu.matmul_pop(first_inner[1]), cp, fld, cells)
    sweep(begin_outer, take_outer, 0, chunks)
    def unpack(from_next, from_prev):
        low = lower(from_next.shape)
        nxt, prv = from_next.astype(F32), from_prev.astype(F32)
        return jnp.where(low, nxt, prv), turned(jnp.where(low, prv, nxt))

    def keep(level, value):
        value = value.astype(BF16)
        rim_m[level] = value[0:members]
        rim_c[level] = value[members : members + group]
        if level < rows:
            rim_p[level] = value[members + group :]

    settle(rt, recv1.at[4])
    for k, (a, b) in enumerate(pairs):
        va, vb = unpack(rt[0, k], rt[1, k])
        keep(a, va)
        keep(b, vb)
    product(half_sum, 0, banded(0, outer, 0), flat_of(rim_m, 0, rows))
    again(first_inner, 0, banded(outer, whole, 0))
    when(-1, lambda: settle(rd.at[0], recv1.at[2]))
    when(1, lambda: settle(rd.at[1], recv1.at[3]))
    for floor in range(2):
        for k in range(half):
            va, vb = unpack(rd[floor, 0, k], rd[floor, 1, k])
            base = rows + floor * HB
            keep(base + k, va)
            keep(base + k + half, vb)
    product(half_sum, 1, banded(0, outer, 2), flat_of(rim_m, rows, window))
    coarse_product(first_inner, rim_c)
    value = pltpu.matmul_pop(half_sum[0]) + pltpu.matmul_pop(half_sum[1])
    put_inner(pltpu.matmul_pop(first_inner[0]), fld_rim, LANE)
    put_outer(value, pltpu.matmul_pop(first_inner[1]), rim_p, fld_rim, LANE)
    rim_fields = jnp.concatenate([fld_rim[0], jnp.zeros((whole, cells - LANE), BF16)], axis=1)
    def rim_of(chunk):
        return square(strip(matrix, chunk, cells, span))

    def begin_rim(chunk):
        into, mxu = slot(chunk)
        product(into[0], mxu, rim_fields[0:outer], rim_of(chunk))
        again(into[1], mxu, rim_fields[outer:])

    begin(late)

    def rim_and_first(chunk):
        value = [strip(matrix, chunk, cells, span), strip(matrix, chunk, 0, LANE)]
        return jnp.concatenate(value, axis=0)

    def second_half(chunk):
        return square(strip(matrix, chunk, LANE, cells))

    def take_rim(chunk, more):
        into, mxu = slot(chunk)
        values = [pltpu.matmul_pop(into[part][mxu]) for part in range(2)]
        if more:
            begin_rim(chunk + 4)
        totals = [[] for _ in range(WIDE)]
        for part in range(2):
            for piece, total in enumerate(summed(values[part], chunk, part)):
                n = chunk * WIDE + piece
                total = total + combined(values[0], piece, part)
                total = total + line[n, part * 8 : part * 8 + 8, :]
                totals[piece].append(total)
                for r, i in enumerate(order[part * 8 : part * 8 + 8]):
                    by = jnp.broadcast_to(total[r : r + 1], (members, LANE)).astype(BF16)
                    at = level_at(i)
                    lanes = slice(n * LANE, (n + 1) * LANE)
                    adj[n, at : at + members, :] = pert[i, :, lanes] * by
        for piece in range(WIDE):
            both = jnp.concatenate(totals[piece], axis=0)
            adj[chunk * WIDE + piece, comb_at:low_at, :] = both.astype(BF16)
        product(rim_sum, mxu, strip(adj, chunk, 0, whole), rim_and_first(chunk), transpose=True)
        product(half_sum, mxu, strip(adj, chunk, 0, outer), second_half(chunk), transpose=True)

    sweep(begin_rim, take_rim, 0, chunks)
    back = pltpu.matmul_pop(rim_sum[0]) + pltpu.matmul_pop(rim_sum[1])
    acc_rim[...] = back[:, 0:LANE]
    acc_own[:, 0:LANE] = back[:, LANE:]
    back = pltpu.matmul_pop(half_sum[0]) + pltpu.matmul_pop(half_sum[1])
    acc_own[0:outer, LANE:] = back[:, 0:LANE]
    out_own[0:edge, :] = acc_own[0:edge, :].astype(BF16)
    out_own[edge:, :] = acc_own[low_at:outer, :].astype(BF16)
    def packed_at(k):
        place = order.index(pairs[k][0])
        entry = place // HB * half + place % HB
        return entry * members + (2 * HB if place >= HB else 0)

    low = lower((members, LANE))
    for k, (a, b) in enumerate(pairs):
        value_a = acc_rim[level_at(a) : level_at(a) + members, :]
        value_b = turned(acc_rim[level_at(b) : level_at(b) + members, :])
        at = slice(packed_at(k), packed_at(k) + members)
        out_rim[1, at, :] = jnp.where(low, value_a, value_b).astype(BF16)
        out_rim[0, at, :] = jnp.where(low, value_b, value_a).astype(BF16)
    for side in range(2):
        both = acc_rim[comb_at:low_at, :].astype(BF16)
        out_rim[side, pcomb_at : pcomb_at + 2 * HB, :] = both[0 : 2 * HB]
        out_rim[side, pinner_at:, :] = both[2 * HB :]

    drain(pk, near + extra + 2 * half * (members + group) * LANE)
    begin([x for x in diag2 + lev2 if x[0] < 0] + tile2)
    for chunk in range(chunks):
        part = strip(adj, chunk, outer, whole)
        product(first_inner, chunk % 2, part, second_half(chunk), transpose=True)
    back = pltpu.matmul_pop(first_inner[0]) + pltpu.matmul_pop(first_inner[1])
    acc_own[outer:, LANE:] = back[:, 0:LANE]
    begin([x for x in diag2 + lev2 if x[0] > 0])
    settle(r_tile, recv2.at[2])
    far = extra + edge * cells + 2 * pedge * LANE
    when(-1, lambda: settle(filler(far), recv2.at[0]))
    when(1, lambda: settle(filler(far), recv2.at[1]))
    def zero_but(value, keep_low):
        low = lower(value.shape)
        return jnp.where(low, value, 0.0) if keep_low else jnp.where(low, 0.0, value)

    def joined(base, messages, at, swap):
        from_prev, from_next = messages[1, at, :].astype(F32), messages[0, at, :].astype(F32)
        if swap:
            from_prev, from_next = turned(from_prev), turned(from_next)
        parts = [base[:, i * LANE : (i + 1) * LANE] for i in range(cells // LANE)]
        parts[0] = parts[0] + zero_but(from_prev, True)
        parts[-1] = parts[-1] + zero_but(from_next, False)
        return parts

    def put(ref, r0, rn, parts):
        for i, part in enumerate(parts):
            ref[r0 : r0 + rn, i * LANE : (i + 1) * LANE] = part.astype(BF16)

    def stored_at(i):
        return (HB + order.index(i)) * members

    for k, pair in enumerate(pairs):
        at = slice(packed_at(k), packed_at(k) + members)
        for swap, i in enumerate(pair):
            base = acc_own[level_at(i) : level_at(i) + members, :]
            put(xm, stored_at(i), members, joined(base, r_tile, at, swap))
    for floor in range(2):
        p0 = o0 = 0 if floor == 0 else 2 * HB
        x0 = 0 if floor == 0 else (HB + rows) * members
        for k in range(half):
            at = slice(p0 + k * members, p0 + (k + 1) * members)
            for swap in range(2):
                i = k + swap * half
                base = r_lev[floor, o0 + i * members : o0 + (i + 1) * members, :].astype(F32)
                put(xm, x0 + i * members, members, joined(base, r_diag.at[floor], at, swap))
    lines, own_lines = [], []
    for floor in (2, 0, 1):
        if floor == 2:
            for p0, a0 in ((pcomb_at, comb_at), (pinner_at, comb_at + 2 * HB)):
                base = acc_own[a0 : a0 + 2 * HB, :]
                own_lines.append(joined(base, r_tile, slice(p0, p0 + 2 * HB), 0))
            for i in range(rows):
                group_at, row = divmod(order.index(i), 2 * HB)
                lines.append([part[row : row + 1] for part in own_lines[group_at]])
            continue
        o0, p0 = (comb_at, pcomb_at) if floor == 0 else (0, 0)
        base = r_lev[floor, o0 : o0 + 2 * HB, :].astype(F32)
        parts = joined(base, r_diag.at[floor], slice(p0, p0 + 2 * HB), 0)
        chosen = range(HB) if floor == 0 else range(HB, 2 * HB)
        lines += [[part[i : i + 1] for part in parts] for i in chosen]
    for level in range(0, window, 2):
        for i in range(cells // LANE):
            lanes = slice(i * LANE, (i + 1) * LANE)
            both = [cp[level + s, :, lanes].astype(F32) * lines[level + s][i] for s in range(2)]
            xc[level * group : (level + 2) * group, lanes] = jnp.concatenate(both, 0).astype(BF16)

    drain(out_rim, edge * cells + 2 * pedge * LANE)


def finish(xm, xc, bm, bc, mo_hbm, co_hbm, mo, co, sem):
    rows, members, cells = mo.shape
    group = co.shape[1]
    copies, pieces = [], 4
    step = rows // pieces
    left = jnp.concatenate([bc[0], bc[1]], axis=1)[:, 0 : xc.shape[0]]
    value = jnp.dot(left, xc[...], preferred_element_type=F32)
    co[...] = value.reshape(rows, group, cells)
    copies.append(pltpu.make_async_copy(co, co_hbm, sem.at[pieces]))
    copies[-1].start()
    for part in range(pieces):
        levels = pl.ds(part * step, step)
        at = slice(part * step * members, (part + 1) * step * members)
        value = jnp.dot(bm[at, :], xm[...], preferred_element_type=F32)
        mo[levels] = value.reshape(step, members, cells)
        copies.append(pltpu.make_async_copy(mo.at[levels], mo_hbm.at[levels], sem.at[part]))
        copies[-1].start()
    for copy in copies:
        copy.wait()


def solution(mesh):
    tiles, levs = mesh.shape["tile"], mesh.shape["lev"]

    def step(members_pert, coarse_pert, member_ctrl, coarse_ctrl, vert_loc, stencil, interp_w):
        rows, members, cells = member_ctrl.shape
        group = coarse_ctrl.shape[1]
        fine = members_pert.shape[2]
        levels, span, lines = rows + 2 * HB, cells + LANE, rows * (members + 1)
        edge = HB * members + 2 * HB
        pedge = HB * members // 2 + 2 * HB
        packed = rows * members // 2 + rows
        hbm = pl.BlockSpec(memory_space=pl.ANY)
        kinds = members + 2 * group
        vmem = pl.BlockSpec(memory_space=pltpu.VMEM)
        results = pl.pallas_call(
            functools.partial(kernel, tiles, levs),
            out_shape=(
                pltpu.VMEM((levels * members, cells), BF16),
                pltpu.VMEM((levels * group, cells), BF16),
                pltpu.VMEM((rows * members, levels * members), BF16),
                pltpu.VMEM((cells // LANE, rows * group, LANE), BF16),
            ),
            in_specs=[hbm] * 7,
            out_specs=(vmem,) * 4,
            scratch_shapes=[
                pltpu.VMEM((levels, members, cells), BF16),
                pltpu.VMEM((levels, group, cells), BF16),
                pltpu.VMEM((levels, group, cells), BF16),
                pltpu.VMEM((rows, members, fine), BF16),
                pltpu.VMEM(vert_loc.shape, F32),
                pltpu.VMEM(stencil.shape, jnp.int32),
                pltpu.VMEM(interp_w.shape, BF16),
                pltpu.VMEM((fine // LANE, span, LANE), BF16),
                pltpu.VMEM((2 * cells // LANE, lines, LANE), BF16),
                pltpu.VMEM((cells // LANE, rows * group, LANE), BF16),
                pltpu.VMEM((levels, members, LANE), BF16),
                pltpu.VMEM((levels, group, LANE), BF16),
                pltpu.VMEM((rows, group, LANE), BF16),
                pltpu.VMEM((2, rows // 2, kinds, LANE), BF16),
                pltpu.VMEM((2, rows // 2, kinds, LANE), BF16),
                pltpu.VMEM((2, 2, HB // 2, members + group, LANE), BF16),
                pltpu.VMEM((cells // LANE, lines, LANE), BF16),
                pltpu.VMEM((1, lines, LANE), BF16),
                pltpu.VMEM((fine // LANE, lines, LANE), BF16),
                pltpu.VMEM((fine // LANE, rows, LANE), F32),
                pltpu.VMEM((lines, LANE), F32),
                pltpu.VMEM((edge + HB * members, cells), BF16),
                pltpu.VMEM((2, packed, LANE), BF16),
                pltpu.VMEM((lines, cells), F32),
                pltpu.VMEM((2, packed, LANE), BF16),
                pltpu.VMEM((2, edge, cells), BF16),
                pltpu.VMEM((2, 2, pedge, LANE), BF16),
                pltpu.SemaphoreType.DMA((5,)),
                pltpu.SemaphoreType.DMA((3,)),
                pltpu.SemaphoreType.DMA((5,)),
                pltpu.SemaphoreType.DMA((3,)),
                pltpu.SemaphoreType.REGULAR((2,)),
            ],
            compiler_params=pltpu.CompilerParams(
                collective_id=0, has_side_effects=True, vmem_limit_bytes=56 * 1024 * 1024
            ),
        )(members_pert, coarse_pert, member_ctrl, coarse_ctrl, vert_loc, stencil, interp_w)
        return pl.pallas_call(
            finish,
            out_shape=(
                jax.ShapeDtypeStruct((rows, members, cells), F32),
                jax.ShapeDtypeStruct((rows, group, cells), F32),
            ),
            in_specs=[vmem] * 4,
            out_specs=(hbm, hbm),
            scratch_shapes=[
                pltpu.VMEM((rows, members, cells), F32),
                pltpu.VMEM((rows, group, cells), F32),
                pltpu.SemaphoreType.DMA((5,)),
            ],
            compiler_params=pltpu.CompilerParams(vmem_limit_bytes=4 * 1024 * 1024),
        )(*results)

    in_specs = (
        P("lev", None, "tile"),
        P("lev", None, "tile"),
        P("lev", None, "tile"),
        P("lev", None, "tile"),
        P(),
        P(None, "tile"),
        P(None, "tile"),
    )
    out_specs = (P("lev", None, "tile"), P("lev", None, "tile"))
    return jax.shard_map(step, mesh=mesh, in_specs=in_specs, out_specs=out_specs, check_vma=False)
```
